32 devices in a mesh: groups: 2 (over y), blk: 4 (over z), sub: 4 (over x, core).
Axes of the slice: x: 2, y: 2, z: 4, core: 2. Of those that a mesh axis runs over, the one named last changes fastest.
Arguments:
- dense_coef: float32 [256, 128, 128], P(('groups', 'blk'), 'sub'), parts along dimension 0, may hold values from -6 to 6
- sparse_coef: float32 [8, 128, 128], P(('groups', 'blk'), 'sub'), parts along dimension 0, may hold values from -0.0234375 to 0.0234375
- pattern: int32 [8], P('groups'), parts along dimension 0, may hold values from 0 to 159, as said below
Outputs:
- product_coef: float32 [256, 128, 128], P(('groups', 'blk'), 'sub'), parts along dimension 0
The draws below stay inside these ranges and needn't reach their ends.
There are 2 independent parts, one for each index of `groups`. The reference program is written for one: setup_inputs(seed, part) draws one part's arguments, and reference() takes and returns one part's arrays. A program takes and returns all parts, laid end to end along the dimension named above; each array names one. Nothing has to cross between parts.
Inputs may be any that keep to these rules, and one draw needn't show every extreme that they name: `pattern`: the 4 entries are distinct.
All inputs are finite; a program needn't handle non-finite values.
Results may differ from the reference program's by a relative error of at most 0.000076.
Values sent between devices are 32-bit elements; how exact they have to be, the bound alone decides.
No kernel may reach another device: no remote copies, remote signals or barrier semaphores. Data moves between devices by JAX's collectives and lax.ppermute only.
A program may use at most 128 MiB of HBM per device.

```python
import jax
import jax.numpy as jnp

ROWS = 128
Q = 128
L = 16384
NT = 128
SB = 160
NNZ = 4


def draw_pattern(key, part):
    order = jax.random.permutation(jax.random.fold_in(key, 7), SB)
    return order[:NNZ].astype(jnp.int32)


def level_of(rng, dims, shards, low, high):
    gain, own = 1.0, jax.random.fold_in(rng, 6)
    for position, parts in shards:
        steps = jnp.exp(jax.random.uniform(jax.random.fold_in(own, position), (parts,), jnp.float32, low / len(shards), high / len(shards)))
        gain = gain * jnp.repeat(steps, dims[position] // parts).reshape([-1 if axis == position else 1 for axis in range(len(dims))])
    return gain


def normal_values(stream_key, shape, scale, limit, split=(), kind=jnp.bfloat16):
    values = scale * jax.random.normal(stream_key, shape, jnp.float32)
    if split:
        values = values * level_of(stream_key, shape, split, -0.22, 0.18)
    return jnp.clip(values, -limit, limit).astype(kind)


def setup_inputs(seed: int = 0, part: int = 0) -> dict:
    streams_of = jax.random.split(jax.random.key(seed), 4)
    own_keys = jax.random.split(jax.random.fold_in(streams_of[3], part), 4)
    dense_coef = normal_values(own_keys[0], (NT, Q, ROWS), 1.0, 6.0, ((0, 4), (1, 4)), jnp.float32)
    sparse_coef = normal_values(own_keys[1], (NNZ, Q, ROWS), (NNZ * L) ** -0.5, 0.0234375, ((0, 4), (1, 4)), jnp.float32)
    pattern = draw_pattern(jax.random.fold_in(jax.random.fold_in(streams_of[3], part), 71), part)
    return {"dense_coef": dense_coef, "sparse_coef": sparse_coef, "pattern": pattern}


def reference(dense_coef, sparse_coef, pattern):
    block_total = dense_coef.shape[0]
    length = ROWS * Q
    dense_flat = jnp.transpose(dense_coef, (0, 2, 1)).reshape(block_total, length)
    sparse_flat = jnp.transpose(sparse_coef, (0, 2, 1)).reshape(sparse_coef.shape[0], length)
    dense_spec = jnp.fft.rfft(dense_flat, n=2 * length, axis=1)
    sparse_spec = jnp.fft.rfft(sparse_flat, n=2 * length, axis=1)
    block_ids = jnp.arange(block_total, dtype=jnp.int32)
    summed = jnp.zeros_like(dense_spec)
    for entry in range(sparse_coef.shape[0]):
        source = jnp.mod(block_ids - pattern[entry].astype(jnp.int32), block_total).astype(jnp.int32)
        summed = summed + jnp.take(dense_spec, source, axis=0) * sparse_spec[entry][None, :]
    product = jnp.fft.irfft(summed, n=2 * length, axis=1)
    result = product[:, :length] + jnp.roll(product[:, length:], 1, axis=0)
    return jnp.transpose(result.reshape(block_total, ROWS, Q), (0, 2, 1)).astype(jnp.float32)
```

```python
import math

import jax
import jax.numpy as jnp
import numpy as np
from jax import lax
from jax.experimental import pallas as pl
from jax.experimental.pallas import tpu as pltpu
from jax.sharding import PartitionSpec as P

LANES = 128
AXES = ("blk", "sub")


def halves(table):
    high = jnp.asarray(table, jnp.float32).astype(jnp.bfloat16)
    low = (jnp.asarray(table, jnp.float32) - high.astype(jnp.float32)).astype(jnp.bfloat16)
    return high, low


def split(values):
    high = values.astype(jnp.bfloat16)
    return high, (values - high.astype(jnp.float32)).astype(jnp.bfloat16)


def product3(left, right, dims):
    dot = lambda a, b: lax.dot_general(a, b, (dims, ((), ())), preferred_element_type=jnp.float32)
    return dot(left[0], right[0]) + (dot(left[0], right[1]) + dot(left[1], right[0]))


def regroup(tiles, width):
    tiles = list(tiles)
    group = lax.broadcasted_iota(jnp.int32, tiles[0].shape, len(tiles[0].shape) - 1) // width
    axis = len(tiles[0].shape) - 1
    step = len(tiles) // 2
    while step:
        keep = (group & step) == 0
        for s in range(len(tiles)):
            if s & step:
                continue
            a, b = tiles[s], tiles[s | step]
            tiles[s] = jnp.where(keep, a, pltpu.roll(b, step * width, axis))
            tiles[s | step] = jnp.where(keep, pltpu.roll(a, LANES - step * width, axis), b)
        step //= 2
    return tiles


class Sizes:
    def __init__(self, dense, sparse, pattern, mesh_shape):
        self.z, self.subs = mesh_shape["blk"], mesh_shape["sub"]
        self.devices = self.z * self.subs
        self.blocks, self.q, self.rows = dense.shape
        self.entries = sparse.shape[0]
        self.all_entries = pattern.shape[0]
        self.nf = self.rows // self.devices
        self.tiles = self.blocks * self.q // LANES
        self.all_blocks = self.blocks * self.z


def tables(n):
    f = np.arange(n.rows) + 0.5
    r = np.arange(n.rows)
    q = np.arange(LANES)
    arm = 2 * math.pi * f[:, None] * r[None, :] / (2 * n.rows)
    order = lambda c, s: np.stack([c.reshape(n.devices, n.nf, -1), s.reshape(n.devices, n.nf, -1)], 1).reshape(2 * n.rows, -1)
    forward = order(np.cos(arm), -np.sin(arm))
    backward = order(np.cos(arm), -np.sin(arm)) / (n.rows * LANES)
    twist = 2 * math.pi * f[:, None] * q[None, :] / (2 * n.rows * LANES)
    twist = np.stack([np.cos(twist), -np.sin(twist)], 0).reshape(2, n.devices, n.nf, LANES)
    turn = 2 * math.pi * (q[:, None] * q[None, :] % LANES) / LANES
    c, s = np.cos(turn), np.sin(turn)
    dft = np.block([[c, -s], [s, c]])
    idft = np.block([[c, s], [-s, c]])
    return forward, backward, twist, dft, idft


def rows_to_slots(n, dense_ref, sparse_ref, high_ref, low_ref, out_ref):
    weights = (high_ref[...], low_ref[...])
    nf = n.nf
    contract = ((1,), (1,))
    group = LANES // n.q
    for t in range(n.tiles):
        part = dense_ref[t * group:(t + 1) * group].reshape(LANES, n.rows)
        slots = product3(weights, split(part), contract)
        for d in range(n.devices):
            for c in range(2):
                out_ref[d, c * n.tiles + t] = slots[(d * 2 + c) * nf:(d * 2 + c + 1) * nf]
    part = sparse_ref[...].reshape(n.entries * n.q, n.rows)
    slots = product3(weights, split(part), contract)
    width = n.entries * n.q
    for d in range(n.devices):
        pieces = [slots[(d * 2 + c) * nf:(d * 2 + c + 1) * nf] for c in range(2)]
        if 2 * width < LANES:
            pieces.append(jnp.zeros((nf, LANES - 2 * width), jnp.float32))
        out_ref[d, 2 * n.tiles] = jnp.concatenate(pieces, axis=1)


def middle(n, place_ref, pattern_ref, in_ref, twist_ref, dft_h, dft_l, idft_h, idft_l, out_ref, wave, spec):
    nf = n.nf
    me = place_ref[0]
    tc, ts = twist_ref[0, me], twist_ref[1, me]
    group = n.subs
    contract = ((1,), (0,))

    def store(index, re, im):
        wave[index, :, :LANES] = re * tc - im * ts
        wave[index, :, LANES:] = re * ts + im * tc

    for z in range(n.z):
        for t in range(n.tiles):
            re = regroup([in_ref[z * n.subs + s, t] for s in range(group)], n.q)
            im = regroup([in_ref[z * n.subs + s, n.tiles + t] for s in range(group)], n.q)
            for j in range(group):
                store(z * n.blocks + t * group + j, re[j], im[j])
        parts = [in_ref[z * n.subs + s, 2 * n.tiles] for s in range(group)]
        width = n.entries * n.q
        for e in range(n.entries):
            at = e * n.q
            re = jnp.concatenate([p[:, at:at + n.q] for p in parts], axis=1)
            im = jnp.concatenate([p[:, width + at:width + at + n.q] for p in parts], axis=1)
            store(n.all_blocks + z * n.entries + e, re, im)

    def transform(source, target, count, table):
        chunk = n.blocks
        starts = list(range(0, count, chunk))
        for at in starts:
            size = min(chunk, count - at)
            rows = source[at:at + size].reshape(size * nf, 2 * LANES)
            target[at:at + size] = product3(split(rows), table, contract).reshape(size, nf, 2 * LANES)

    transform(wave, spec, n.all_blocks + n.all_entries, (dft_h[...], dft_l[...]))

    shifts = [lax.rem(pattern_ref[e], n.all_blocks) for e in range(n.all_entries)]
    first = me * nf
    slot = lax.broadcasted_iota(jnp.int32, (nf, LANES), 0) + first
    sign = jnp.where(lax.rem(slot, 2) == 0, 1.0, -1.0).astype(jnp.float32)

    def convolved(k):
        re = jnp.zeros((nf, LANES), jnp.float32)
        im = jnp.zeros((nf, LANES), jnp.float32)
        for e in range(n.all_entries):
            j = k - shifts[e]
            j = jnp.where(j < 0, j + n.all_blocks, j)
            ar, ai = spec[j, :, :LANES], spec[j, :, LANES:]
            sr, si = spec[n.all_blocks + e, :, :LANES], spec[n.all_blocks + e, :, LANES:]
            re = re + ar * sr - ai * si
            im = im + ar * si + ai * sr
        return re, im

    def step(k, before):
        re, im = convolved(k)
        wave[k, :, :LANES] = re - sign * before[1]
        wave[k, :, LANES:] = im + sign * before[0]
        return re, im

    lax.fori_loop(0, n.all_blocks, step, convolved(n.all_blocks - 1), unroll=8)

    transform(wave, spec, n.all_blocks, (idft_h[...], idft_l[...]))

    for z in range(n.z):
        for t in range(n.tiles):
            re, im = [], []
            for j in range(group):
                index = z * n.blocks + t * group + j
                er, ei = spec[index, :, :LANES], spec[index, :, LANES:]
                re.append(er * tc + ei * ts)
                im.append(ei * tc - er * ts)
            for s, tile in enumerate(regroup(re, n.q)):
                out_ref[z * n.subs + s, t] = tile
            for s, tile in enumerate(regroup(im, n.q)):
                out_ref[z * n.subs + s, n.tiles + t] = tile


def slots_to_rows(n, in_ref, high_ref, low_ref, out_ref):
    weights = (high_ref[...], low_ref[...])
    group = LANES // n.q
    for t in range(n.tiles):
        pieces = [in_ref[d, c * n.tiles + t] for d in range(n.devices) for c in range(2)]
        slots = jnp.concatenate(pieces, axis=0)
        rows = product3(split(slots), weights, ((0,), (0,)))
        out_ref[t * group:(t + 1) * group] = rows.reshape(group, n.q, n.rows)


def solution(mesh):
    def local(dense, sparse, pattern):
        n = Sizes(dense, sparse, pattern, mesh.shape)
        forward, backward, twist, dft, idft = tables(n)
        place = (lax.axis_index("blk") * n.subs + lax.axis_index("sub")).reshape(1)
        scalar = pl.BlockSpec(memory_space=pltpu.SMEM)
        whole = pl.BlockSpec(memory_space=pltpu.VMEM)
        out = lambda *shape: jax.ShapeDtypeStruct(shape, jnp.float32)
        sent = pl.pallas_call(
            lambda *refs: rows_to_slots(n, *refs),
            out_shape=out(n.devices, 2 * n.tiles + 1, n.nf, LANES),
            in_specs=[whole] * 4, out_specs=whole, name="rows_to_slots",
        )(dense, sparse, *halves(forward))
        taken = lax.all_to_all(sent, AXES, 0, 0, tiled=True)
        mixed = pl.pallas_call(
            lambda *refs: middle(n, *refs),
            out_shape=out(n.devices, 2 * n.tiles, n.nf, LANES),
            in_specs=[scalar] * 2 + [whole] * 6, out_specs=whole, name="middle",
            scratch_shapes=[pltpu.VMEM((n.all_blocks + n.all_entries, n.nf, 2 * LANES), jnp.float32)] * 2,
        )(place, pattern, taken, jnp.asarray(twist, jnp.float32), *halves(dft), *halves(idft))
        back = lax.all_to_all(mixed, AXES, 0, 0, tiled=True)
        return pl.pallas_call(
            lambda *refs: slots_to_rows(n, *refs),
            out_shape=out(*dense.shape),
            in_specs=[whole] * 3, out_specs=whole, name="slots_to_rows",
        )(back, *halves(backward))

    return jax.shard_map(
        local,
        mesh=mesh,
        in_specs=(P(("groups", "blk"), "sub", None), P(("groups", "blk"), "sub", None), P("groups")),
        out_specs=P(("groups", "blk"), "sub", None),
        check_vma=False,
    )
```

```python
import math

import jax
import jax.numpy as jnp
import numpy as np
from jax import lax
from jax.experimental import pallas as pl
from jax.experimental.pallas import tpu as pltpu
from jax.sharding import PartitionSpec as P

LANES = 128
GRANT = pltpu.CompilerParams(vmem_limit_bytes=16 * 2**20)
AXES = ("blk", "sub")


def halves(table):
    table = np.asarray(table, np.float32)
    high = table.astype(jnp.bfloat16)
    low = (table - high.astype(np.float32)).astype(jnp.bfloat16)
    return high, low


def split(values):
    high = values.astype(jnp.bfloat16)
    return high, (values - high.astype(jnp.float32)).astype(jnp.bfloat16)


def product3(left, right, dims):
    dot = lambda a, b: lax.dot_general(a, b, (dims, ((), ())), preferred_element_type=jnp.float32)
    return dot(left[0], right[0]) + (dot(left[0], right[1]) + dot(left[1], right[0]))


def regroup(tiles, width):
    tiles = list(tiles)
    group = lax.broadcasted_iota(jnp.int32, tiles[0].shape, len(tiles[0].shape) - 1) // width
    axis = len(tiles[0].shape) - 1
    step = len(tiles) // 2
    while step:
        keep = (group & step) == 0
        for s in range(len(tiles)):
            if s & step:
                continue
            a, b = tiles[s], tiles[s | step]
            tiles[s] = jnp.where(keep, a, pltpu.roll(b, step * width, axis))
            tiles[s | step] = jnp.where(keep, pltpu.roll(a, LANES - step * width, axis), b)
        step //= 2
    return tiles


class Sizes:
    def __init__(self, dense, sparse, pattern, mesh_shape):
        self.z, self.subs = mesh_shape["blk"], mesh_shape["sub"]
        self.devices = self.z * self.subs
        self.blocks, self.q, self.rows = dense.shape
        self.entries = sparse.shape[0]
        self.all_entries = pattern.shape[0]
        self.nf = self.rows // self.devices
        self.tiles = self.blocks * self.q // LANES
        self.all_blocks = self.blocks * self.z


def tables(n):
    f = np.arange(n.rows) + 0.5
    r = np.arange(n.rows)
    q = np.arange(LANES)
    arm = 2 * math.pi * f[:, None] * r[None, :] / (2 * n.rows)
    order = lambda c, s: np.stack([c.reshape(n.devices, n.nf, -1), s.reshape(n.devices, n.nf, -1)], 1).reshape(2 * n.rows, -1)
    forward = order(np.cos(arm), -np.sin(arm))
    backward = order(np.cos(arm), -np.sin(arm)) / (n.rows * LANES)
    twist = 2 * math.pi * f[:, None] * q[None, :] / (2 * n.rows * LANES)
    twist = np.stack([np.cos(twist), -np.sin(twist)], 0).reshape(2, n.devices, n.nf, LANES)
    turn = 2 * math.pi * (q[:, None] * q[None, :] % LANES) / LANES
    c, s = np.cos(turn), np.sin(turn)
    dft = np.block([[c, -s], [s, c]])
    idft = np.block([[c, s], [-s, c]])
    return forward, backward, twist, dft, idft


def rows_to_slots(n, dense_hbm, sparse_hbm, weights_hbm, out_ref, dense, sparse, weights, sems):
    nf = n.nf
    contract = ((1,), (1,))
    group = LANES // n.q
    width = n.entries * n.q
    steps = min(4, n.tiles)
    per = n.tiles // steps
    loads = [pltpu.make_async_copy(weights_hbm, weights, sems.at[0])]
    for s in range(steps):
        part = pl.ds(s * per * group, per * group)
        loads.append(pltpu.make_async_copy(dense_hbm.at[part], dense.at[part], sems.at[1 + s]))
    loads.append(pltpu.make_async_copy(sparse_hbm, sparse, sems.at[1 + steps]))
    for load in loads:
        load.start()
    loads[0].wait()
    table = (weights[0], weights[1])
    for s in range(steps):
        loads[1 + s].wait()
        for t in range(s * per, (s + 1) * per):
            part = dense[t * group:(t + 1) * group].reshape(LANES, n.rows)
            slots = product3(table, split(part), contract)
            for d in range(n.devices):
                for c in range(2):
                    out_ref[d, c * n.tiles + t] = slots[(d * 2 + c) * nf:(d * 2 + c + 1) * nf]
    loads[-1].wait()
    slots = product3(table, split(sparse[...].reshape(width, n.rows)), contract)
    for d in range(n.devices):
        pieces = [slots[(d * 2 + c) * nf:(d * 2 + c + 1) * nf] for c in range(2)]
        if 2 * width < LANES:
            pieces.append(jnp.zeros((nf, LANES - 2 * width), jnp.float32))
        out_ref[d, 2 * n.tiles] = jnp.concatenate(pieces, axis=1)


def middle(n, pattern_ref, in_ref, twist_ref, dft_h, dft_l, idft_h, idft_l, out_ref, wave, spec):
    nf = n.nf
    me = lax.axis_index("blk") * n.subs + lax.axis_index("sub")
    tc, ts = twist_ref[0, me], twist_ref[1, me]
    group = n.subs
    contract = ((1,), (0,))

    def store(index, re, im):
        wave[index, :, :LANES] = re * tc - im * ts
        wave[index, :, LANES:] = re * ts + im * tc

    for z in range(n.z):
        for t in range(n.tiles):
            re = regroup([in_ref[z * n.subs + s, t] for s in range(group)], n.q)
            im = regroup([in_ref[z * n.subs + s, n.tiles + t] for s in range(group)], n.q)
            for j in range(group):
                store(z * n.blocks + t * group + j, re[j], im[j])
        parts = [in_ref[z * n.subs + s, 2 * n.tiles] for s in range(group)]
        width = n.entries * n.q
        for e in range(n.entries):
            at = e * n.q
            re = jnp.concatenate([p[:, at:at + n.q] for p in parts], axis=1)
            im = jnp.concatenate([p[:, width + at:width + at + n.q] for p in parts], axis=1)
            store(n.all_blocks + z * n.entries + e, re, im)

    def transform(source, target, count, table):
        chunk = n.blocks
        starts = list(range(0, count, chunk))
        for at in starts:
            size = min(chunk, count - at)
            rows = source[at:at + size].reshape(size * nf, 2 * LANES)
            target[at:at + size] = product3(split(rows), table, contract).reshape(size, nf, 2 * LANES)

    transform(wave, spec, n.all_blocks + n.all_entries, (dft_h[...], dft_l[...]))

    shifts = [lax.rem(pattern_ref[e], n.all_blocks) for e in range(n.all_entries)]
    first = me * nf
    slot = lax.broadcasted_iota(jnp.int32, (nf, LANES), 0) + first
    sign = jnp.where(lax.rem(slot, 2) == 0, 1.0, -1.0).astype(jnp.float32)

    def convolved(k):
        re = jnp.zeros((nf, LANES), jnp.float32)
        im = jnp.zeros((nf, LANES), jnp.float32)
        for e in range(n.all_entries):
            j = k - shifts[e]
            if n.all_blocks & (n.all_blocks - 1) == 0:
                j = j & (n.all_blocks - 1)
            else:
                j = jnp.where(j < 0, j + n.all_blocks, j)
            ar, ai = spec[j, :, :LANES], spec[j, :, LANES:]
            sr, si = spec[n.all_blocks + e, :, :LANES], spec[n.all_blocks + e, :, LANES:]
            re = re + ar * sr - ai * si
            im = im + ar * si + ai * sr
        return re, im

    def step(k, before):
        re, im = convolved(k)
        wave[k, :, :LANES] = re - sign * before[1]
        wave[k, :, LANES:] = im + sign * before[0]
        return re, im

    lax.fori_loop(0, n.all_blocks, step, convolved(n.all_blocks - 1), unroll=8)

    transform(wave, spec, n.all_blocks, (idft_h[...], idft_l[...]))

    for z in range(n.z):
        for t in range(n.tiles):
            re, im = [], []
            for j in range(group):
                index = z * n.blocks + t * group + j
                er, ei = spec[index, :, :LANES], spec[index, :, LANES:]
                re.append(er * tc + ei * ts)
                im.append(ei * tc - er * ts)
            for s, tile in enumerate(regroup(re, n.q)):
                out_ref[z * n.subs + s, t] = tile
            for s, tile in enumerate(regroup(im, n.q)):
                out_ref[z * n.subs + s, n.tiles + t] = tile


def slots_to_rows(n, in_ref, weights_ref, out_hbm, rows_ref, sems):
    weights = (weights_ref[0], weights_ref[1])
    group = LANES // n.q
    steps = min(4, n.tiles)
    per = n.tiles // steps
    stores = []
    for s in range(steps):
        for t in range(s * per, (s + 1) * per):
            pieces = [in_ref[d, c * n.tiles + t] for d in range(n.devices) for c in range(2)]
            slots = jnp.concatenate(pieces, axis=0)
            rows = product3(split(slots), weights, ((0,), (0,)))
            rows_ref[t * group:(t + 1) * group] = rows.reshape(group, n.q, n.rows)
        part = pl.ds(s * per * group, per * group)
        stores.append(pltpu.make_async_copy(rows_ref.at[part], out_hbm.at[part], sems.at[s]))
        stores[-1].start()
    for store in stores:
        store.wait()


def solution(mesh):
    def local(dense, sparse, pattern):
        n = Sizes(dense, sparse, pattern, mesh.shape)
        forward, backward, twist, dft, idft = tables(n)
        scalar = pl.BlockSpec(memory_space=pltpu.SMEM)
        whole = pl.BlockSpec(memory_space=pltpu.VMEM)
        out = lambda *shape: jax.ShapeDtypeStruct(shape, jnp.float32)
        hbm = pl.BlockSpec(memory_space=pltpu.HBM)
        steps = min(4, n.tiles)
        sent = pl.pallas_call(
            lambda *refs: rows_to_slots(n, *refs),
            out_shape=pltpu.VMEM((n.devices, 2 * n.tiles + 1, n.nf, LANES), jnp.float32),
            in_specs=[hbm] * 3, out_specs=whole, name="rows_to_slots", compiler_params=GRANT,
            scratch_shapes=[
                pltpu.VMEM(dense.shape, jnp.float32), pltpu.VMEM(sparse.shape, jnp.float32),
                pltpu.VMEM((2, *forward.shape), jnp.bfloat16), pltpu.SemaphoreType.DMA((steps + 2,)),
            ],
        )(*(pltpu.with_memory_space_constraint(v, pltpu.HBM) for v in (dense, sparse, jnp.stack([jnp.asarray(h) for h in halves(forward)]))))
        taken = lax.all_to_all(sent, AXES, 0, 0, tiled=True)
        mixed = pl.pallas_call(
            lambda *refs: middle(n, *refs),
            out_shape=out(n.devices, 2 * n.tiles, n.nf, LANES),
            in_specs=[scalar] + [whole] * 6, out_specs=whole, name="middle", compiler_params=GRANT,
            scratch_shapes=[pltpu.VMEM((n.all_blocks + n.all_entries, n.nf, 2 * LANES), jnp.float32)] * 2,
        )(pattern, taken, jnp.asarray(twist, jnp.float32), *halves(dft), *halves(idft))
        back = lax.all_to_all(mixed, AXES, 0, 0, tiled=True)
        return pl.pallas_call(
            lambda *refs: slots_to_rows(n, *refs),
            out_shape=out(*dense.shape),
            in_specs=[whole] * 2, out_specs=hbm, name="slots_to_rows", compiler_params=GRANT,
            scratch_shapes=[pltpu.VMEM(dense.shape, jnp.float32), pltpu.SemaphoreType.DMA((steps,))],
        )(back, np.stack(halves(backward)))

    return jax.shard_map(
        local,
        mesh=mesh,
        in_specs=(P(("groups", "blk"), "sub", None), P(("groups", "blk"), "sub", None), P("groups")),
        out_specs=P(("groups", "blk"), "sub", None),
        check_vma=False,
    )
```

```python
import math

import jax
import jax.numpy as jnp
import numpy as np
from jax import lax
from jax.experimental import pallas as pl
from jax.experimental.pallas import tpu as pltpu
from jax.sharding import PartitionSpec as P

LANES = 128
GRANT = pltpu.CompilerParams(vmem_limit_bytes=16 * 2**20)
AXES = ("blk", "sub")


def halves(table):
    table = np.asarray(table, np.float32)
    high = table.astype(jnp.bfloat16)
    low = (table - high.astype(np.float32)).astype(jnp.bfloat16)
    return high, low


def split(values):
    high = values.astype(jnp.bfloat16)
    return high, (values - high.astype(jnp.float32)).astype(jnp.bfloat16)


def product3(left, right, dims):
    dot = lambda a, b: lax.dot_general(a, b, (dims, ((), ())), preferred_element_type=jnp.float32)
    return dot(left[0], right[0]) + (dot(left[0], right[1]) + dot(left[1], right[0]))


def regroup(tiles, width):
    tiles = list(tiles)
    group = lax.broadcasted_iota(jnp.int32, tiles[0].shape, len(tiles[0].shape) - 1) // width
    axis = len(tiles[0].shape) - 1
    step = len(tiles) // 2
    while step:
        keep = (group & step) == 0
        for s in range(len(tiles)):
            if s & step:
                continue
            a, b = tiles[s], tiles[s | step]
            tiles[s] = jnp.where(keep, a, pltpu.roll(b, step * width, axis))
            tiles[s | step] = jnp.where(keep, pltpu.roll(a, LANES - step * width, axis), b)
        step //= 2
    return tiles


class Sizes:
    def __init__(self, dense, sparse, pattern, mesh_shape):
        self.z, self.subs = mesh_shape["blk"], mesh_shape["sub"]
        self.devices = self.z * self.subs
        self.blocks, self.q, self.rows = dense.shape
        self.entries = sparse.shape[0]
        self.all_entries = pattern.shape[0]
        self.nf = self.rows // self.devices
        self.tiles = self.blocks * self.q // LANES
        self.all_blocks = self.blocks * self.z


def tables(n):
    f = np.arange(n.rows) + 0.5
    r = np.arange(n.rows)
    q = np.arange(LANES)
    arm = 2 * math.pi * f[:, None] * r[None, :] / (2 * n.rows)
    order = lambda c, s: np.stack([c.reshape(n.devices, n.nf, -1), s.reshape(n.devices, n.nf, -1)], 1).reshape(2 * n.rows, -1)
    forward = order(np.cos(arm), -np.sin(arm))
    backward = order(np.cos(arm), -np.sin(arm)) / (n.rows * LANES)
    twist = 2 * math.pi * f[:, None] * q[None, :] / (2 * n.rows * LANES)
    twist = np.stack([np.cos(twist), -np.sin(twist)], 0).reshape(2, n.devices, n.nf, LANES)
    turn = 2 * math.pi * (q[:, None] * q[None, :] % LANES) / LANES
    c, s = np.cos(turn), np.sin(turn)
    dft = np.block([[c, -s], [s, c]])
    idft = np.block([[c, s], [-s, c]])
    return forward, backward, twist, dft, idft


def rows_to_slots(n, dense_hbm, sparse_hbm, weights_hbm, out_ref, dense, sparse, weights, sems):
    nf = n.nf
    contract = ((1,), (1,))
    group = LANES // n.q
    width = n.entries * n.q
    steps = min(4, n.tiles)
    per = n.tiles // steps
    loads = [pltpu.make_async_copy(weights_hbm, weights, sems.at[0])]
    for s in range(steps):
        part = pl.ds(s * per * group, per * group)
        loads.append(pltpu.make_async_copy(dense_hbm.at[part], dense.at[part], sems.at[1 + s]))
    loads.append(pltpu.make_async_copy(sparse_hbm, sparse, sems.at[1 + steps]))
    for load in loads:
        load.start()
    loads[0].wait()
    table = weights[...]

    def slots_of(rows):
        high, low = split(rows)
        both = jnp.concatenate([high, low], axis=1)
        dot = lambda x, y: lax.dot_general(x, y, (contract, ((), ())), preferred_element_type=jnp.float32)
        return dot(table[:, :2 * n.rows], both) + dot(table[:, 2 * n.rows:], high)

    for s in range(steps):
        loads[1 + s].wait()
        slots = slots_of(dense[s * per * group:(s + 1) * per * group].reshape(per * LANES, n.rows))
        for i in range(per):
            t = s * per + i
            for d in range(n.devices):
                for c in range(2):
                    rows = slice((d * 2 + c) * nf, (d * 2 + c + 1) * nf)
                    out_ref[d, c * n.tiles + t] = slots[rows, i * LANES:(i + 1) * LANES]
    loads[-1].wait()
    slots = slots_of(sparse[...].reshape(width, n.rows))
    for d in range(n.devices):
        pieces = [slots[(d * 2 + c) * nf:(d * 2 + c + 1) * nf] for c in range(2)]
        if 2 * width < LANES:
            pieces.append(jnp.zeros((nf, LANES - 2 * width), jnp.float32))
        out_ref[d, 2 * n.tiles] = jnp.concatenate(pieces, axis=1)


RUN = 8


def middle(n, pattern_ref, in_ref, twist_ref, dft_h, dft_l, idft_h, idft_l, out_ref, wave, spec):
    nf = n.nf
    me = lax.axis_index("blk") * n.subs + lax.axis_index("sub")
    tc, ts = twist_ref[0, me], twist_ref[1, me]
    group = n.subs
    contract = ((1,), (0,))
    base = n.all_entries
    width = n.entries * n.q

    def store(index, re, im):
        wave[index, :, :LANES] = re * tc - im * ts
        wave[index, :, LANES:] = re * ts + im * tc

    def transform(at, count, table):
        rows = wave[at:at + count].reshape(count * nf, 2 * LANES)
        return product3(split(rows), table, contract).reshape(count, nf, 2 * LANES)

    def gather(z):
        if z == 0:
            for y in range(n.z):
                parts = [in_ref[y * n.subs + s, 2 * n.tiles] for s in range(group)]
                for e in range(n.entries):
                    at = e * n.q
                    re = jnp.concatenate([p[:, at:at + n.q] for p in parts], axis=1)
                    im = jnp.concatenate([p[:, width + at:width + at + n.q] for p in parts], axis=1)
                    store(y * n.entries + e, re, im)
        for t in range(n.tiles):
            re = regroup([in_ref[z * n.subs + s, t] for s in range(group)], n.q)
            im = regroup([in_ref[z * n.subs + s, n.tiles + t] for s in range(group)], n.q)
            for j in range(group):
                store(base + z * n.blocks + t * group + j, re[j], im[j])

    def forward(z):
        at = base + z * n.blocks if z else 0
        count = n.blocks if z else base + n.blocks
        result = transform(at, count, (dft_h[...], dft_l[...]))
        re, im = result[:, :, :LANES], result[:, :, LANES:]
        spec[at:at + count, :, :LANES] = re
        spec[at:at + count, :, LANES:2 * LANES] = im
        spec[at:at + count, :, 2 * LANES:] = re + im

    gather(0)
    for z in range(1, n.z):
        gather(z)
        forward(z - 1)
    forward(n.z - 1)
    spec[base + n.all_blocks:base + n.all_blocks + RUN] = spec[base:base + RUN]

    shifts = [lax.rem(pattern_ref[e], n.all_blocks) for e in range(n.all_entries)]
    slot = lax.broadcasted_iota(jnp.int32, (nf, LANES), 0) + me * nf
    sign = jnp.where(lax.rem(slot, 2) == 0, 1.0, -1.0).astype(jnp.float32)

    def factors():
        out = []
        for e in range(n.all_entries):
            sr, si = spec[e, :, :LANES], spec[e, :, LANES:2 * LANES]
            out.append((sr, si + sr, si - sr))
        return out

    def starts(k):
        out = []
        for shift in shifts:
            j = k - shift
            out.append(base + jnp.where(j < 0, j + n.all_blocks, j))
        return out

    def convolved(rows, i, table):
        t = u = v = None
        for e, (sr, ssum, sdiff) in enumerate(table):
            at = rows[e] + i
            a = spec[at, :, 2 * LANES:] * sr
            b = spec[at, :, LANES:2 * LANES] * ssum
            c = spec[at, :, :LANES] * sdiff
            t, u, v = (a, b, c) if t is None else (t + a, u + b, v + c)
        return t - u, t + v

    def run_of(k, before, table):
        rows = starts(k)
        for i in range(RUN):
            re, im = convolved(rows, i, table)
            wave[k + i, :, :LANES] = re - sign * before[1]
            wave[k + i, :, LANES:] = im + sign * before[0]
            before = (re, im)
        return before

    def convolve(z, before):
        if n.all_blocks * n.all_entries <= 1024:
            table = factors()
            for k in range(z * n.blocks, (z + 1) * n.blocks, RUN):
                before = run_of(k, before, table)
            return before
        return lax.fori_loop(
            0, n.blocks // RUN,
            lambda i, carry: run_of(z * n.blocks + i * RUN, carry, factors()), before)

    def scatter(z):
        result = transform(z * n.blocks, n.blocks, (idft_h[...], idft_l[...]))
        for t in range(n.tiles):
            re, im = [], []
            for j in range(group):
                er, ei = result[t * group + j, :, :LANES], result[t * group + j, :, LANES:]
                re.append(er * tc + ei * ts)
                im.append(ei * tc - er * ts)
            for s, tile in enumerate(regroup(re, n.q)):
                out_ref[z * n.subs + s, t] = tile
            for s, tile in enumerate(regroup(im, n.q)):
                out_ref[z * n.subs + s, n.tiles + t] = tile

    before = convolved(starts(n.all_blocks - 1), 0, factors())
    before = convolve(0, before)
    for z in range(1, n.z):
        before = convolve(z, before)
        scatter(z - 1)
    scatter(n.z - 1)


def slots_to_rows(n, in_ref, weights_ref, out_hbm, rows_ref, sems):
    both = weights_ref[...]
    first = both[:, :n.rows]
    group = LANES // n.q
    steps = min(8, n.tiles)
    per = n.tiles // steps
    dot = lambda a, b: lax.dot_general(a, b, (((0,), (0,)), ((), ())), preferred_element_type=jnp.float32)
    stores = []
    for s in range(steps):
        for t in range(s * per, (s + 1) * per):
            pieces = [in_ref[d, c * n.tiles + t] for d in range(n.devices) for c in range(2)]
            high, low = split(jnp.concatenate(pieces, axis=0))
            wide = dot(high, both)
            rows = wide[:, :n.rows] + (wide[:, n.rows:] + dot(low, first))
            rows_ref[t * group:(t + 1) * group] = rows.reshape(group, n.q, n.rows)
        part = pl.ds(s * per * group, per * group)
        stores.append(pltpu.make_async_copy(rows_ref.at[part], out_hbm.at[part], sems.at[s]))
        stores[-1].start()
    for store in stores:
        store.wait()


def solution(mesh):
    def local(dense, sparse, pattern):
        n = Sizes(dense, sparse, pattern, mesh.shape)
        forward, backward, twist, dft, idft = tables(n)
        scalar = pl.BlockSpec(memory_space=pltpu.SMEM)
        whole = pl.BlockSpec(memory_space=pltpu.VMEM)
        out = lambda *shape: jax.ShapeDtypeStruct(shape, jnp.float32)
        hbm = pl.BlockSpec(memory_space=pltpu.HBM)
        steps = min(4, n.tiles)
        high, low = halves(forward)
        table = np.concatenate([high, high, low], axis=1)
        sent = pl.pallas_call(
            lambda *refs: rows_to_slots(n, *refs),
            out_shape=pltpu.VMEM((n.devices, 2 * n.tiles + 1, n.nf, LANES), jnp.float32),
            in_specs=[hbm] * 3, out_specs=whole, name="rows_to_slots", compiler_params=GRANT,
            scratch_shapes=[
                pltpu.VMEM(dense.shape, jnp.float32), pltpu.VMEM(sparse.shape, jnp.float32),
                pltpu.VMEM((2 * n.rows, 3 * n.rows), jnp.bfloat16), pltpu.SemaphoreType.DMA((steps + 2,)),
            ],
        )(*(pltpu.with_memory_space_constraint(v, pltpu.HBM) for v in (dense, sparse, jnp.asarray(table))))
        taken = lax.all_to_all(sent, AXES, 0, 0, tiled=True)
        mixed = pl.pallas_call(
            lambda *refs: middle(n, *refs),
            out_shape=out(n.devices, 2 * n.tiles, n.nf, LANES),
            in_specs=[scalar] + [whole] * 6, out_specs=whole, name="middle", compiler_params=GRANT,
            scratch_shapes=[
                pltpu.VMEM((n.all_entries + n.all_blocks, n.nf, 2 * LANES), jnp.float32),
                pltpu.VMEM((n.all_entries + n.all_blocks + RUN, n.nf, 3 * LANES), jnp.float32),
            ],
        )(pattern, taken, jnp.asarray(twist, jnp.float32), *halves(dft), *halves(idft))
        back = lax.all_to_all(mixed, AXES, 0, 0, tiled=True)
        return pl.pallas_call(
            lambda *refs: slots_to_rows(n, *refs),
            out_shape=out(*dense.shape),
            in_specs=[whole] * 2, out_specs=hbm, name="slots_to_rows", compiler_params=GRANT,
            scratch_shapes=[pltpu.VMEM(dense.shape, jnp.float32), pltpu.SemaphoreType.DMA((min(8, n.tiles),))],
        )(back, np.concatenate(halves(backward), axis=1))

    return jax.shard_map(
        local,
        mesh=mesh,
        in_specs=(P(("groups", "blk"), "sub", None), P(("groups", "blk"), "sub", None), P("groups")),
        out_specs=P(("groups", "blk"), "sub", None),
        check_vma=False,
    )
```

```python
import math

import jax
import jax.numpy as jnp
import numpy as np
from jax import lax
from jax.experimental import pallas as pl
from jax.experimental.pallas import tpu as pltpu
from jax.sharding import PartitionSpec as P

LANES = 128
GRANT = pltpu.CompilerParams(vmem_limit_bytes=16 * 2**20)
AXES = ("blk", "sub")


def halves(table):
    table = np.asarray(table, np.float32)
    high = table.astype(jnp.bfloat16)
    low = (table - high.astype(np.float32)).astype(jnp.bfloat16)
    return high, low


def split(values):
    high = values.astype(jnp.bfloat16)
    return high, (values - high.astype(jnp.float32)).astype(jnp.bfloat16)


def product3(left, right, dims):
    dot = lambda a, b: lax.dot_general(a, b, (dims, ((), ())), preferred_element_type=jnp.float32)
    return dot(left[0], right[0]) + (dot(left[0], right[1]) + dot(left[1], right[0]))


def regroup(tiles, width):
    count = len(tiles)
    group = lax.broadcasted_iota(jnp.int32, tiles[0].shape, len(tiles[0].shape) - 1) // width
    tiles = list(tiles)
    step = 1
    while step < count:
        keep = (group & step) == 0
        tiles = [jnp.where(keep, tiles[m], tiles[(m + step) % count]) for m in range(count)]
        step *= 2
    return [tiles[-j % count] for j in range(count)]


class Sizes:
    def __init__(self, dense, sparse, pattern, mesh_shape):
        self.z, self.subs = mesh_shape["blk"], mesh_shape["sub"]
        self.devices = self.z * self.subs
        self.blocks, self.q, self.rows = dense.shape
        self.entries = sparse.shape[0]
        self.all_entries = pattern.shape[0]
        self.nf = self.rows // self.devices
        self.tiles = self.blocks * self.q // LANES
        self.all_blocks = self.blocks * self.z


def tables(n):
    f = np.arange(n.rows) + 0.5
    r = np.arange(n.rows)
    q = np.arange(LANES)
    arm = 2 * math.pi * f[:, None] * r[None, :] / (2 * n.rows)
    order = lambda c, s: np.stack([c.reshape(n.devices, n.nf, -1), s.reshape(n.devices, n.nf, -1)], 1).reshape(2 * n.rows, -1)
    forward = order(np.cos(arm), -np.sin(arm))
    backward = order(np.cos(arm), -np.sin(arm)) / (n.rows * LANES)
    twist = 2 * math.pi * f[:, None] * q[None, :] / (2 * n.rows * LANES)
    twist = np.stack([np.cos(twist), -np.sin(twist)], 0).reshape(2, n.devices, n.nf, LANES)
    turn = 2 * math.pi * (q[:, None] * q[None, :] % LANES) / LANES
    c, s = np.cos(turn), np.sin(turn)
    dft = np.block([[c, -s], [s, c]])
    idft = np.block([[c, s], [-s, c]])
    phase = 2 * math.pi * (np.arange(n.subs)[:, None] * q[None, :] % n.subs) / n.subs
    phase = np.stack([np.cos(phase), -np.sin(phase)], 0).reshape(2, n.subs, 1, LANES)
    return forward, backward, phase, twist, dft, idft


def rows_to_slots(n, dense_hbm, sparse_hbm, weights_hbm, out_ref, dense, sparse, weights, sems):
    nf = n.nf
    contract = ((1,), (1,))
    group = LANES // n.q
    width = n.entries * n.q
    steps = min(4, n.tiles)
    per = n.tiles // steps
    loads = [pltpu.make_async_copy(weights_hbm, weights, sems.at[0])]
    for s in range(steps):
        part = pl.ds(s * per * group, per * group)
        loads.append(pltpu.make_async_copy(dense_hbm.at[part], dense.at[part], sems.at[1 + s]))
    loads.append(pltpu.make_async_copy(sparse_hbm, sparse, sems.at[1 + steps]))
    for load in loads:
        load.start()
    loads[0].wait()
    table = weights[...]
    me = lax.axis_index("sub")

    def slots_of(rows):
        high, low = split(rows)
        both = jnp.concatenate([high, low], axis=1)
        dot = lambda x, y: lax.dot_general(x, y, (contract, ((), ())), preferred_element_type=jnp.float32)
        return dot(table[:, :2 * n.rows], both) + dot(table[:, 2 * n.rows:], high)

    for s in range(steps):
        loads[1 + s].wait()
        rows = [
            dense[t * group + lax.rem(g - me + group, group)]
            for t in range(s * per, (s + 1) * per) for g in range(group)
        ]
        slots = slots_of(jnp.concatenate(rows, axis=0))
        for i in range(per):
            t = s * per + i
            for d in range(n.devices):
                for c in range(2):
                    rows = slice((d * 2 + c) * nf, (d * 2 + c + 1) * nf)
                    out_ref[d, c * n.tiles + t] = slots[rows, i * LANES:(i + 1) * LANES]
    loads[-1].wait()
    slots = slots_of(sparse[...].reshape(width, n.rows))
    for d in range(n.devices):
        pieces = [slots[(d * 2 + c) * nf:(d * 2 + c + 1) * nf] for c in range(2)]
        if 2 * width < LANES:
            pieces.append(jnp.zeros((nf, LANES - 2 * width), jnp.float32))
        out_ref[d, 2 * n.tiles] = jnp.concatenate(pieces, axis=1)


RUN = 8


def middle(n, pattern_ref, in_ref, phase_ref, twist_ref, dft_h, dft_l, idft_h, idft_l, out_ref, wave, spec):
    nf = n.nf
    me = lax.axis_index("blk") * n.subs + lax.axis_index("sub")
    group = n.subs
    turned = [[twist_ref[c, me] if j == 0 else pltpu.roll(twist_ref[c, me], j * n.q, 1) for c in range(2)] for j in range(group)]
    contract = ((1,), (0,))
    base = n.all_entries
    width = n.entries * n.q

    def store(index, re, im, j=0):
        tc, ts = turned[j]
        wave[index, :, :LANES] = re * tc - im * ts
        wave[index, :, LANES:] = re * ts + im * tc

    def transform(at, count, table):
        rows = wave[at:at + count].reshape(count * nf, 2 * LANES)
        return product3(split(rows), table, contract).reshape(count, nf, 2 * LANES)

    def gather(z):
        if z == 0:
            for y in range(n.z):
                parts = [in_ref[y * n.subs + s, 2 * n.tiles] for s in range(group)]
                for e in range(n.entries):
                    at = e * n.q
                    re = jnp.concatenate([p[:, at:at + n.q] for p in parts], axis=1)
                    im = jnp.concatenate([p[:, width + at:width + at + n.q] for p in parts], axis=1)
                    store(y * n.entries + e, re, im)
        for t in range(n.tiles):
            re = regroup([in_ref[z * n.subs + s, t] for s in range(group)], n.q)
            im = regroup([in_ref[z * n.subs + s, n.tiles + t] for s in range(group)], n.q)
            for j in range(group):
                store(base + z * n.blocks + t * group + j, re[j], im[j], j)

    def forward(z):
        at = base + z * n.blocks if z else 0
        count = n.blocks if z else base + n.blocks
        result = transform(at, count, (dft_h[...], dft_l[...]))
        re, im = result[:, :, :LANES], result[:, :, LANES:]
        spec[at:at + count, :, :LANES] = re
        spec[at:at + count, :, LANES:2 * LANES] = im
        spec[at:at + count, :, 2 * LANES:] = re + im

    gather(0)
    for z in range(1, n.z):
        gather(z)
        forward(z - 1)
    forward(n.z - 1)
    spec[base + n.all_blocks:base + n.all_blocks + RUN] = spec[base:base + RUN]

    shifts = [lax.rem(pattern_ref[e], n.all_blocks) for e in range(n.all_entries)]
    slot = lax.broadcasted_iota(jnp.int32, (nf, LANES), 0) + me * nf
    sign = jnp.where(lax.rem(slot, 2) == 0, 1.0, -1.0).astype(jnp.float32)
    over_re, over_im = -sign * phase_ref[1, 1], sign * phase_ref[0, 1]

    def factors():
        out = []
        for e in range(n.all_entries):
            xr, xi = spec[e, :, :LANES], spec[e, :, LANES:2 * LANES]
            power = lax.rem(shifts[e], group)
            pr, pi = phase_ref[0, power], phase_ref[1, power]
            sr, si = xr * pr - xi * pi, xr * pi + xi * pr
            out.append((sr, si + sr, si - sr))
        return out

    def starts(k):
        out = []
        for shift in shifts:
            j = k - shift
            out.append(base + jnp.where(j < 0, j + n.all_blocks, j))
        return out

    def convolved(rows, i, table):
        t = u = v = None
        for e, (sr, ssum, sdiff) in enumerate(table):
            at = rows[e] + i
            a = spec[at, :, 2 * LANES:] * sr
            b = spec[at, :, LANES:2 * LANES] * ssum
            c = spec[at, :, :LANES] * sdiff
            t, u, v = (a, b, c) if t is None else (t + a, u + b, v + c)
        return t - u, t + v

    def run_of(k, before, table):
        rows = starts(k)
        for i in range(RUN):
            re, im = convolved(rows, i, table)
            wave[k + i, :, :LANES] = re + (over_re * before[0] - over_im * before[1])
            wave[k + i, :, LANES:] = im + (over_re * before[1] + over_im * before[0])
            before = (re, im)
        return before

    def convolve(z, before):
        if n.all_blocks * n.all_entries <= 1024:
            table = factors()
            for k in range(z * n.blocks, (z + 1) * n.blocks, RUN):
                before = run_of(k, before, table)
            return before
        return lax.fori_loop(
            0, n.blocks // RUN,
            lambda i, carry: run_of(z * n.blocks + i * RUN, carry, factors()), before)

    def scatter(z):
        result = transform(z * n.blocks, n.blocks, (idft_h[...], idft_l[...]))
        for t in range(n.tiles):
            re, im = [], []
            for j in range(group):
                tc, ts = turned[j]
                er, ei = result[t * group + j, :, :LANES], result[t * group + j, :, LANES:]
                re.append(er * tc + ei * ts)
                im.append(ei * tc - er * ts)
            for s, tile in enumerate(regroup(re, n.q)):
                out_ref[z * n.subs + s, t] = tile
            for s, tile in enumerate(regroup(im, n.q)):
                out_ref[z * n.subs + s, n.tiles + t] = tile

    before = convolved(starts(n.all_blocks - 1), 0, factors())
    before = convolve(0, before)
    for z in range(1, n.z):
        before = convolve(z, before)
        scatter(z - 1)
    scatter(n.z - 1)


def slots_to_rows(n, in_ref, weights_ref, out_hbm, rows_ref, sems):
    both = weights_ref[...]
    first = both[:, :n.rows]
    group = LANES // n.q
    me = lax.axis_index("sub")
    steps = min(8, n.tiles)
    per = n.tiles // steps
    dot = lambda a, b: lax.dot_general(a, b, (((0,), (0,)), ((), ())), preferred_element_type=jnp.float32)
    stores = []
    for s in range(steps):
        for t in range(s * per, (s + 1) * per):
            pieces = [in_ref[d, c * n.tiles + t] for d in range(n.devices) for c in range(2)]
            high, low = split(jnp.concatenate(pieces, axis=0))
            wide = dot(high, both)
            rows = wide[:, :n.rows] + (wide[:, n.rows:] + dot(low, first))
            for g in range(group):
                rows_ref[t * group + lax.rem(g - me + group, group)] = rows[g * n.q:(g + 1) * n.q]
        part = pl.ds(s * per * group, per * group)
        stores.append(pltpu.make_async_copy(rows_ref.at[part], out_hbm.at[part], sems.at[s]))
        stores[-1].start()
    for store in stores:
        store.wait()


def solution(mesh):
    def local(dense, sparse, pattern):
        n = Sizes(dense, sparse, pattern, mesh.shape)
        forward, backward, phase, twist, dft, idft = tables(n)
        scalar = pl.BlockSpec(memory_space=pltpu.SMEM)
        whole = pl.BlockSpec(memory_space=pltpu.VMEM)
        out = lambda *shape: jax.ShapeDtypeStruct(shape, jnp.float32)
        hbm = pl.BlockSpec(memory_space=pltpu.HBM)
        steps = min(4, n.tiles)
        high, low = halves(forward)
        table = np.concatenate([high, high, low], axis=1)
        sent = pl.pallas_call(
            lambda *refs: rows_to_slots(n, *refs),
            out_shape=pltpu.VMEM((n.devices, 2 * n.tiles + 1, n.nf, LANES), jnp.float32),
            in_specs=[hbm] * 3, out_specs=whole, name="rows_to_slots", compiler_params=GRANT,
            scratch_shapes=[
                pltpu.VMEM(dense.shape, jnp.float32), pltpu.VMEM(sparse.shape, jnp.float32),
                pltpu.VMEM((2 * n.rows, 3 * n.rows), jnp.bfloat16), pltpu.SemaphoreType.DMA((steps + 2,)),
            ],
        )(*(pltpu.with_memory_space_constraint(v, pltpu.HBM) for v in (dense, sparse, jnp.asarray(table))))
        taken = lax.all_to_all(sent, AXES, 0, 0, tiled=True)
        mixed = pl.pallas_call(
            lambda *refs: middle(n, *refs),
            out_shape=out(n.devices, 2 * n.tiles, n.nf, LANES),
            in_specs=[scalar] + [whole] * 7, out_specs=whole, name="middle", compiler_params=GRANT,
            scratch_shapes=[
                pltpu.VMEM((n.all_entries + n.all_blocks, n.nf, 2 * LANES), jnp.float32),
                pltpu.VMEM((n.all_entries + n.all_blocks + RUN, n.nf, 3 * LANES), jnp.float32),
            ],
        )(pattern, taken, jnp.asarray(phase, jnp.float32), jnp.asarray(twist, jnp.float32), *halves(dft), *halves(idft))
        back = lax.all_to_all(mixed, AXES, 0, 0, tiled=True)
        return pl.pallas_call(
            lambda *refs: slots_to_rows(n, *refs),
            out_shape=out(*dense.shape),
            in_specs=[whole] * 2, out_specs=hbm, name="slots_to_rows", compiler_params=GRANT,
            scratch_shapes=[pltpu.VMEM(dense.shape, jnp.float32), pltpu.SemaphoreType.DMA((min(8, n.tiles),))],
        )(back, np.concatenate(halves(backward), axis=1))

    return jax.shard_map(
        local,
        mesh=mesh,
        in_specs=(P(("groups", "blk"), "sub", None), P(("groups", "blk"), "sub", None), P("groups")),
        out_specs=P(("groups", "blk"), "sub", None),
        check_vma=False,
    )
```

```python
import math

import jax
import jax.numpy as jnp
import numpy as np
from jax import lax
from jax.experimental import pallas as pl
from jax.experimental.pallas import tpu as pltpu
from jax.sharding import PartitionSpec as P

LANES = 128
GRANT = pltpu.CompilerParams(vmem_limit_bytes=16 * 2**20)
AXES = ("blk", "sub")


def halves(table):
    table = np.asarray(table, np.float32)
    high = table.astype(jnp.bfloat16)
    low = (table - high.astype(np.float32)).astype(jnp.bfloat16)
    return high, low


def split(values):
    high = values.astype(jnp.bfloat16)
    return high, (values - high.astype(jnp.float32)).astype(jnp.bfloat16)


def product3(left, right, dims):
    dot = lambda a, b: lax.dot_general(a, b, (dims, ((), ())), preferred_element_type=jnp.float32)
    return dot(left[0], right[0]) + (dot(left[0], right[1]) + dot(left[1], right[0]))


def regroup(tiles, width):
    count = len(tiles)
    group = lax.broadcasted_iota(jnp.int32, tiles[0].shape, len(tiles[0].shape) - 1) // width
    tiles = list(tiles)
    step = 1
    while step < count:
        keep = (group & step) == 0
        tiles = [jnp.where(keep, tiles[m], tiles[(m + step) % count]) for m in range(count)]
        step *= 2
    return [tiles[-j % count] for j in range(count)]


class Sizes:
    def __init__(self, dense, sparse, pattern, mesh_shape):
        self.z, self.subs = mesh_shape["blk"], mesh_shape["sub"]
        self.devices = self.z * self.subs
        self.blocks, self.q, self.rows = dense.shape
        self.entries = sparse.shape[0]
        self.all_entries = pattern.shape[0]
        self.nf = self.rows // self.devices
        self.tiles = self.blocks * self.q // LANES
        self.all_blocks = self.blocks * self.z


def tables(n):
    f = np.arange(n.rows) + 0.5
    r = np.arange(n.rows)
    q = np.arange(LANES)
    arm = 2 * math.pi * f[:, None] * r[None, :] / (2 * n.rows)
    order = lambda c, s: np.stack([c.reshape(n.devices, n.nf, -1), s.reshape(n.devices, n.nf, -1)], 1).reshape(2 * n.rows, -1)
    forward = order(np.cos(arm), -np.sin(arm))
    backward = order(np.cos(arm), -np.sin(arm)) / (n.rows * LANES)
    twist = 2 * math.pi * f[:, None] * q[None, :] / (2 * n.rows * LANES)
    twist = np.stack([np.cos(twist), -np.sin(twist)], 0).reshape(2, n.devices, n.nf, LANES)
    turn = 2 * math.pi * (q[:, None] * q[None, :] % LANES) / LANES
    c, s = np.cos(turn), np.sin(turn)
    dft = np.block([[c, -s], [s, c]])
    idft = np.block([[c, s], [-s, c]])
    phase = 2 * math.pi * (np.arange(n.subs)[:, None] * q[None, :] % n.subs) / n.subs
    phase = np.stack([np.cos(phase), -np.sin(phase)], 0).reshape(2, n.subs, 1, LANES)
    return forward, backward, phase, twist, dft, idft


def rows_to_slots(n, dense_hbm, sparse_hbm, weights_hbm, out_ref, dense, sparse, weights, sems):
    nf = n.nf
    contract = ((1,), (1,))
    group = LANES // n.q
    width = n.entries * n.q
    loads = [
        pltpu.make_async_copy(weights_hbm, weights, sems.at[0]),
        pltpu.make_async_copy(sparse_hbm, sparse, sems.at[1]),
        pltpu.make_async_copy(dense_hbm, dense, sems.at[2]),
    ]
    for load in loads:
        load.start()
    for load in loads:
        load.wait()
    first, second = weights[:, :n.rows], weights[:, n.rows:]
    twice = jnp.concatenate([first, first], axis=1)
    me = lax.axis_index("sub")

    def slots_of(rows):
        high, low = split(rows)
        both = jnp.concatenate([high, low], axis=1)
        dot = lambda x, y: lax.dot_general(x, y, (contract, ((), ())), preferred_element_type=jnp.float32)
        return dot(twice, both) + dot(second, high)

    few = slots_of(sparse[...].reshape(width, n.rows))
    for d in range(n.devices):
        pieces = [few[(d * 2 + c) * nf:(d * 2 + c + 1) * nf] for c in range(2)]
        if 2 * width < LANES:
            pieces.append(jnp.zeros((nf, LANES - 2 * width), jnp.float32))
        out_ref[d, 2 * n.tiles] = jnp.concatenate(pieces, axis=1)
    rows = [dense[t * group + lax.rem(g - me + group, group)] for t in range(n.tiles) for g in range(group)]
    slots = slots_of(jnp.concatenate(rows, axis=0))
    for t in range(n.tiles):
        for d in range(n.devices):
            for c in range(2):
                at = slice((d * 2 + c) * nf, (d * 2 + c + 1) * nf)
                out_ref[d, c * n.tiles + t] = slots[at, t * LANES:(t + 1) * LANES]


RUN = 8


def middle(n, pattern_ref, in_ref, phase_ref, twist_ref, dft_h, dft_l, idft_h, idft_l, out_ref, wave, spec):
    nf = n.nf
    me = lax.axis_index("blk") * n.subs + lax.axis_index("sub")
    group = n.subs
    turned = [[twist_ref[c, me] if j == 0 else pltpu.roll(twist_ref[c, me], j * n.q, 1) for c in range(2)] for j in range(group)]
    contract = ((1,), (0,))
    base = n.all_entries
    width = n.entries * n.q

    def store(index, re, im, j=0):
        tc, ts = turned[j]
        wave[index, :, :LANES] = re * tc - im * ts
        wave[index, :, LANES:] = re * ts + im * tc

    def transform(at, count, table):
        rows = wave[at:at + count].reshape(count * nf, 2 * LANES)
        return product3(split(rows), table, contract).reshape(count, nf, 2 * LANES)

    def gather(z):
        if z == 0:
            for y in range(n.z):
                parts = [in_ref[y * n.subs + s, 2 * n.tiles] for s in range(group)]
                for e in range(n.entries):
                    at = e * n.q
                    re = jnp.concatenate([p[:, at:at + n.q] for p in parts], axis=1)
                    im = jnp.concatenate([p[:, width + at:width + at + n.q] for p in parts], axis=1)
                    store(y * n.entries + e, re, im)
        for t in range(n.tiles):
            re = regroup([in_ref[z * n.subs + s, t] for s in range(group)], n.q)
            im = regroup([in_ref[z * n.subs + s, n.tiles + t] for s in range(group)], n.q)
            for j in range(group):
                store(base + z * n.blocks + t * group + j, re[j], im[j], j)

    def forward(z):
        at = base + z * n.blocks if z else 0
        count = n.blocks if z else base + n.blocks
        result = transform(at, count, (dft_h[...], dft_l[...]))
        re, im = result[:, :, :LANES], result[:, :, LANES:]
        spec[at:at + count, :, :LANES] = re
        spec[at:at + count, :, LANES:2 * LANES] = im
        spec[at:at + count, :, 2 * LANES:] = re + im

    gather(0)
    for z in range(1, n.z):
        gather(z)
        forward(z - 1)
    forward(n.z - 1)
    spec[base + n.all_blocks:base + n.all_blocks + RUN] = spec[base:base + RUN]

    shifts = [lax.rem(pattern_ref[e], n.all_blocks) for e in range(n.all_entries)]
    slot = lax.broadcasted_iota(jnp.int32, (nf, LANES), 0) + me * nf
    sign = jnp.where(lax.rem(slot, 2) == 0, 1.0, -1.0).astype(jnp.float32)
    over_re, over_im = -sign * phase_ref[1, 1], sign * phase_ref[0, 1]

    def factors():
        out = []
        for e in range(n.all_entries):
            xr, xi = spec[e, :, :LANES], spec[e, :, LANES:2 * LANES]
            power = lax.rem(shifts[e], group)
            pr, pi = phase_ref[0, power], phase_ref[1, power]
            sr, si = xr * pr - xi * pi, xr * pi + xi * pr
            out.append((sr, si + sr, si - sr))
        return out

    def starts(k):
        out = []
        for shift in shifts:
            j = k - shift
            out.append(base + jnp.where(j < 0, j + n.all_blocks, j))
        return out

    def convolved(rows, i, table):
        t = u = v = None
        for e, (sr, ssum, sdiff) in enumerate(table):
            at = rows[e] + i
            a = spec[at, :, 2 * LANES:] * sr
            b = spec[at, :, LANES:2 * LANES] * ssum
            c = spec[at, :, :LANES] * sdiff
            t, u, v = (a, b, c) if t is None else (t + a, u + b, v + c)
        return t - u, t + v

    def run_of(k, before, table):
        rows = starts(k)
        for i in range(RUN):
            re, im = convolved(rows, i, table)
            wave[k + i, :, :LANES] = re + (over_re * before[0] - over_im * before[1])
            wave[k + i, :, LANES:] = im + (over_re * before[1] + over_im * before[0])
            before = (re, im)
        return before

    def convolve(z, before):
        if n.all_blocks * n.all_entries <= 1024:
            table = factors()
            for k in range(z * n.blocks, (z + 1) * n.blocks, RUN):
                before = run_of(k, before, table)
            return before
        return lax.fori_loop(
            0, n.blocks // RUN,
            lambda i, carry: run_of(z * n.blocks + i * RUN, carry, factors()), before)

    def scatter(z):
        result = transform(z * n.blocks, n.blocks, (idft_h[...], idft_l[...]))
        for t in range(n.tiles):
            re, im = [], []
            for j in range(group):
                tc, ts = turned[j]
                er, ei = result[t * group + j, :, :LANES], result[t * group + j, :, LANES:]
                re.append(er * tc + ei * ts)
                im.append(ei * tc - er * ts)
            for s, tile in enumerate(regroup(re, n.q)):
                out_ref[z * n.subs + s, t] = tile
            for s, tile in enumerate(regroup(im, n.q)):
                out_ref[z * n.subs + s, n.tiles + t] = tile

    before = convolved(starts(n.all_blocks - 1), 0, factors())
    before = convolve(0, before)
    for z in range(1, n.z):
        before = convolve(z, before)
        scatter(z - 1)
    scatter(n.z - 1)


def slots_to_rows(n, in_ref, weights_ref, out_hbm, rows_ref, sems):
    both = weights_ref[...]
    first = both[:, :n.rows]
    group = LANES // n.q
    me = lax.axis_index("sub")
    steps = min(8, n.tiles)
    per = n.tiles // steps
    dot = lambda a, b: lax.dot_general(a, b, (((0,), (0,)), ((), ())), preferred_element_type=jnp.float32)
    stores = []
    for s in range(steps):
        for t in range(s * per, (s + 1) * per):
            pieces = [in_ref[d, c * n.tiles + t] for d in range(n.devices) for c in range(2)]
            high, low = split(jnp.concatenate(pieces, axis=0))
            wide = dot(high, both)
            rows = wide[:, :n.rows] + (wide[:, n.rows:] + dot(low, first))
            for g in range(group):
                rows_ref[t * group + lax.rem(g - me + group, group)] = rows[g * n.q:(g + 1) * n.q]
        part = pl.ds(s * per * group, per * group)
        stores.append(pltpu.make_async_copy(rows_ref.at[part], out_hbm.at[part], sems.at[s]))
        stores[-1].start()
    for store in stores:
        store.wait()


def solution(mesh):
    def local(dense, sparse, pattern):
        n = Sizes(dense, sparse, pattern, mesh.shape)
        forward, backward, phase, twist, dft, idft = tables(n)
        scalar = pl.BlockSpec(memory_space=pltpu.SMEM)
        whole = pl.BlockSpec(memory_space=pltpu.VMEM)
        out = lambda *shape: jax.ShapeDtypeStruct(shape, jnp.float32)
        hbm = pl.BlockSpec(memory_space=pltpu.HBM)
        high, low = halves(forward)
        table = np.concatenate([high, low], axis=1)
        sent = pl.pallas_call(
            lambda *refs: rows_to_slots(n, *refs),
            out_shape=pltpu.VMEM((n.devices, 2 * n.tiles + 1, n.nf, LANES), jnp.float32),
            in_specs=[hbm] * 3, out_specs=whole, name="rows_to_slots", compiler_params=GRANT,
            scratch_shapes=[
                pltpu.VMEM(dense.shape, jnp.float32), pltpu.VMEM(sparse.shape, jnp.float32),
                pltpu.VMEM((2 * n.rows, 2 * n.rows), jnp.bfloat16), pltpu.SemaphoreType.DMA((3,)),
            ],
        )(*(pltpu.with_memory_space_constraint(v, pltpu.HBM) for v in (dense, sparse, jnp.asarray(table))))
        taken = lax.all_to_all(sent, AXES, 0, 0, tiled=True)
        mixed = pl.pallas_call(
            lambda *refs: middle(n, *refs),
            out_shape=out(n.devices, 2 * n.tiles, n.nf, LANES),
            in_specs=[scalar] + [whole] * 7, out_specs=whole, name="middle", compiler_params=GRANT,
            scratch_shapes=[
                pltpu.VMEM((n.all_entries + n.all_blocks, n.nf, 2 * LANES), jnp.float32),
                pltpu.VMEM((n.all_entries + n.all_blocks + RUN, n.nf, 3 * LANES), jnp.float32),
            ],
        )(pattern, taken, jnp.asarray(phase, jnp.float32), jnp.asarray(twist, jnp.float32), *halves(dft), *halves(idft))
        back = lax.all_to_all(mixed, AXES, 0, 0, tiled=True)
        return pl.pallas_call(
            lambda *refs: slots_to_rows(n, *refs),
            out_shape=out(*dense.shape),
            in_specs=[whole] * 2, out_specs=hbm, name="slots_to_rows", compiler_params=GRANT,
            scratch_shapes=[pltpu.VMEM(dense.shape, jnp.float32), pltpu.SemaphoreType.DMA((min(8, n.tiles),))],
        )(back, np.concatenate(halves(backward), axis=1))

    return jax.shard_map(
        local,
        mesh=mesh,
        in_specs=(P(("groups", "blk"), "sub", None), P(("groups", "blk"), "sub", None), P("groups")),
        out_specs=P(("groups", "blk"), "sub", None),
        check_vma=False,
    )
```

```python
import math

import jax
import jax.numpy as jnp
import numpy as np
from jax import lax
from jax.experimental import pallas as pl
from jax.experimental.pallas import tpu as pltpu
from jax.sharding import PartitionSpec as P

LANES = 128
GRANT = pltpu.CompilerParams(vmem_limit_bytes=16 * 2**20)
AXES = ("blk", "sub")


def halves(table):
    table = np.asarray(table, np.float32)
    high = table.astype(jnp.bfloat16)
    low = (table - high.astype(np.float32)).astype(jnp.bfloat16)
    return high, low


def split(values):
    high = values.astype(jnp.bfloat16)
    return high, (values - high.astype(jnp.float32)).astype(jnp.bfloat16)


def product3(left, right, dims):
    dot = lambda a, b: lax.dot_general(a, b, (dims, ((), ())), preferred_element_type=jnp.float32)
    return dot(left[0], right[0]) + (dot(left[0], right[1]) + dot(left[1], right[0]))


def regroup(tiles, width):
    count = len(tiles)
    group = lax.broadcasted_iota(jnp.int32, tiles[0].shape, len(tiles[0].shape) - 1) // width
    tiles = list(tiles)
    step = 1
    while step < count:
        keep = (group & step) == 0
        tiles = [jnp.where(keep, tiles[m], tiles[(m + step) % count]) for m in range(count)]
        step *= 2
    return [tiles[-j % count] for j in range(count)]


class Sizes:
    def __init__(self, dense, sparse, pattern, mesh_shape):
        self.z, self.subs = mesh_shape["blk"], mesh_shape["sub"]
        self.devices = self.z * self.subs
        self.blocks, self.q, self.rows = dense.shape
        self.entries = sparse.shape[0]
        self.all_entries = pattern.shape[0]
        self.nf = self.rows // self.devices
        self.tiles = self.blocks * self.q // LANES
        self.all_blocks = self.blocks * self.z
        self.parts = 2 if self.nf % 2 == 0 and 4 * self.entries * self.q <= LANES else 1
        self.height = self.nf // self.parts
        self.pieces = (2 * self.tiles) * self.parts + 1


def tables(n):
    f = np.arange(n.rows) + 0.5
    r = np.arange(n.rows)
    q = np.arange(LANES)
    arm = 2 * math.pi * f[:, None] * r[None, :] / (2 * n.rows)
    order = lambda c, s: np.stack([c.reshape(n.devices, n.nf, -1), s.reshape(n.devices, n.nf, -1)], 1).reshape(2 * n.rows, -1)
    forward = order(np.cos(arm), -np.sin(arm))
    backward = order(np.cos(arm), -np.sin(arm)) / (n.rows * LANES)
    twist = 2 * math.pi * f[:, None] * q[None, :] / (2 * n.rows * LANES)
    twist = np.stack([np.cos(twist), -np.sin(twist)], 0).reshape(2, n.devices, n.nf, LANES)
    turn = 2 * math.pi * (q[:, None] * q[None, :] % LANES) / LANES
    c, s = np.cos(turn), np.sin(turn)
    dft = np.block([[c, -s], [s, c]])
    idft = np.block([[c, s], [-s, c]])
    phase = 2 * math.pi * (np.arange(n.subs)[:, None] * q[None, :] % n.subs) / n.subs
    phase = np.stack([np.cos(phase), -np.sin(phase)], 0).reshape(2, n.subs, 1, LANES)
    return forward, backward, phase, twist, dft, idft


def rows_to_slots(n, dense_hbm, sparse_hbm, weights_hbm, out_ref, dense, sparse, weights, sems):
    nf = n.nf
    contract = ((1,), (1,))
    group = LANES // n.q
    width = n.entries * n.q
    loads = [
        pltpu.make_async_copy(weights_hbm, weights, sems.at[0]),
        pltpu.make_async_copy(sparse_hbm, sparse, sems.at[1]),
        pltpu.make_async_copy(dense_hbm, dense, sems.at[2]),
    ]
    for load in loads:
        load.start()
    for load in loads:
        load.wait()
    first, second = weights[:, :n.rows], weights[:, n.rows:]
    twice = jnp.concatenate([first, first], axis=1)
    me = lax.axis_index("sub")

    def slots_of(rows):
        high, low = split(rows)
        both = jnp.concatenate([high, low], axis=1)
        dot = lambda x, y: lax.dot_general(x, y, (contract, ((), ())), preferred_element_type=jnp.float32)
        return dot(twice, both) + dot(second, high)

    few = slots_of(sparse[...].reshape(width, n.rows))
    for d in range(n.devices):
        pieces = []
        for p in range(n.parts):
            for c in range(2):
                at = (d * 2 + c) * nf + p * n.height
                pieces.append(few[at:at + n.height])
        if 2 * n.parts * width < LANES:
            pieces.append(jnp.zeros((n.height, LANES - 2 * n.parts * width), jnp.float32))
        out_ref[d, n.pieces - 1] = jnp.concatenate(pieces, axis=1)
    rows = [dense[t * group + lax.rem(g - me + group, group)] for t in range(n.tiles) for g in range(group)]
    slots = slots_of(jnp.concatenate(rows, axis=0))
    for t in range(n.tiles):
        for d in range(n.devices):
            for c in range(2):
                at = (d * 2 + c) * nf
                tile = slots[at:at + nf, t * LANES:(t + 1) * LANES]
                first_piece = (c * n.tiles + t) * n.parts
                out_ref[d, first_piece:first_piece + n.parts] = tile.reshape(n.parts, n.height, LANES)


RUN = 8


def middle(n, pattern_ref, in_ref, phase_ref, twist_ref, dft_h, dft_l, idft_h, idft_l, out_ref, wave, spec):
    nf = n.nf
    me = lax.axis_index("blk") * n.subs + lax.axis_index("sub")
    group = n.subs
    turned = [[twist_ref[c, me] if j == 0 else pltpu.roll(twist_ref[c, me], j * n.q, 1) for c in range(2)] for j in range(group)]
    contract = ((1,), (0,))
    base = n.all_entries
    width = n.entries * n.q

    def store(index, re, im, j=0):
        tc, ts = turned[j]
        wave[index, :, :LANES] = re * tc - im * ts
        wave[index, :, LANES:] = re * ts + im * tc

    def transform(at, count, table):
        rows = wave[at:at + count].reshape(count * nf, 2 * LANES)
        return product3(split(rows), table, contract).reshape(count, nf, 2 * LANES)

    def tile(source, i):
        return in_ref[source, i * n.parts:(i + 1) * n.parts].reshape(nf, LANES)

    def gather(z):
        if z == 0:
            for y in range(n.z):
                few = [in_ref[y * n.subs + s, n.pieces - 1] for s in range(group)]
                for e in range(n.entries):
                    re, im = (
                        jnp.concatenate([
                            jnp.concatenate([
                                v[:, (p * 2 + c) * width + e * n.q:(p * 2 + c) * width + (e + 1) * n.q]
                                for v in few], axis=1)
                            for p in range(n.parts)], axis=0)
                        for c in range(2))
                    store(y * n.entries + e, re, im)
        for t in range(n.tiles):
            re = regroup([tile(z * n.subs + s, t) for s in range(group)], n.q)
            im = regroup([tile(z * n.subs + s, n.tiles + t) for s in range(group)], n.q)
            for j in range(group):
                store(base + z * n.blocks + t * group + j, re[j], im[j], j)

    def forward(z):
        at = base + z * n.blocks if z else 0
        count = n.blocks if z else base + n.blocks
        result = transform(at, count, (dft_h[...], dft_l[...]))
        re, im = result[:, :, :LANES], result[:, :, LANES:]
        spec[at:at + count, :, :LANES] = re
        spec[at:at + count, :, LANES:2 * LANES] = im
        spec[at:at + count, :, 2 * LANES:] = re + im

    gather(0)
    for z in range(1, n.z):
        gather(z)
        forward(z - 1)
    forward(n.z - 1)
    spec[base + n.all_blocks:base + n.all_blocks + RUN] = spec[base:base + RUN]

    shifts = [lax.rem(pattern_ref[e], n.all_blocks) for e in range(n.all_entries)]
    slot = lax.broadcasted_iota(jnp.int32, (nf, LANES), 0) + me * nf
    sign = jnp.where(lax.rem(slot, 2) == 0, 1.0, -1.0).astype(jnp.float32)
    over_re, over_im = -sign * phase_ref[1, 1], sign * phase_ref[0, 1]

    def factors():
        out = []
        for e in range(n.all_entries):
            xr, xi = spec[e, :, :LANES], spec[e, :, LANES:2 * LANES]
            power = lax.rem(shifts[e], group)
            pr, pi = phase_ref[0, power], phase_ref[1, power]
            sr, si = xr * pr - xi * pi, xr * pi + xi * pr
            out.append((sr, si + sr, si - sr))
        return out

    def starts(k):
        out = []
        for shift in shifts:
            j = k - shift
            out.append(base + jnp.where(j < 0, j + n.all_blocks, j))
        return out

    def convolved(rows, i, table):
        t = u = v = None
        for e, (sr, ssum, sdiff) in enumerate(table):
            at = rows[e] + i
            a = spec[at, :, 2 * LANES:] * sr
            b = spec[at, :, LANES:2 * LANES] * ssum
            c = spec[at, :, :LANES] * sdiff
            t, u, v = (a, b, c) if t is None else (t + a, u + b, v + c)
        return t - u, t + v

    def run_of(k, before, table):
        rows = starts(k)
        for i in range(RUN):
            re, im = convolved(rows, i, table)
            wave[k + i, :, :LANES] = re + (over_re * before[0] - over_im * before[1])
            wave[k + i, :, LANES:] = im + (over_re * before[1] + over_im * before[0])
            before = (re, im)
        return before

    def convolve(z, before):
        if n.all_blocks * n.all_entries <= 1024:
            table = factors()
            for k in range(z * n.blocks, (z + 1) * n.blocks, RUN):
                before = run_of(k, before, table)
            return before
        return lax.fori_loop(
            0, n.blocks // RUN,
            lambda i, carry: run_of(z * n.blocks + i * RUN, carry, factors()), before)

    def scatter(z):
        result = transform(z * n.blocks, n.blocks, (idft_h[...], idft_l[...]))
        for t in range(n.tiles):
            re, im = [], []
            for j in range(group):
                tc, ts = turned[j]
                er, ei = result[t * group + j, :, :LANES], result[t * group + j, :, LANES:]
                re.append(er * tc + ei * ts)
                im.append(ei * tc - er * ts)
            for s, value in enumerate(regroup(re, n.q)):
                out_ref[z * n.subs + s, t] = value
            for s, value in enumerate(regroup(im, n.q)):
                out_ref[z * n.subs + s, n.tiles + t] = value

    before = convolved(starts(n.all_blocks - 1), 0, factors())
    before = convolve(0, before)
    for z in range(1, n.z):
        before = convolve(z, before)
        scatter(z - 1)
    scatter(n.z - 1)


def slots_to_rows(n, in_ref, weights_ref, out_hbm, rows_ref, sems):
    both = weights_ref[...]
    first = both[:, :n.rows]
    group = LANES // n.q
    me = lax.axis_index("sub")
    steps = min(8, n.tiles)
    per = n.tiles // steps
    dot = lambda a, b: lax.dot_general(a, b, (((0,), (0,)), ((), ())), preferred_element_type=jnp.float32)
    stores = []
    for s in range(steps):
        for t in range(s * per, (s + 1) * per):
            pieces = [in_ref[d, c * n.tiles + t] for d in range(n.devices) for c in range(2)]
            high, low = split(jnp.concatenate(pieces, axis=0))
            wide = dot(high, both)
            rows = wide[:, :n.rows] + (wide[:, n.rows:] + dot(low, first))
            for g in range(group):
                rows_ref[t * group + lax.rem(g - me + group, group)] = rows[g * n.q:(g + 1) * n.q]
        part = pl.ds(s * per * group, per * group)
        stores.append(pltpu.make_async_copy(rows_ref.at[part], out_hbm.at[part], sems.at[s]))
        stores[-1].start()
    for store in stores:
        store.wait()


def solution(mesh):
    def local(dense, sparse, pattern):
        n = Sizes(dense, sparse, pattern, mesh.shape)
        forward, backward, phase, twist, dft, idft = tables(n)
        scalar = pl.BlockSpec(memory_space=pltpu.SMEM)
        whole = pl.BlockSpec(memory_space=pltpu.VMEM)
        out = lambda *shape: jax.ShapeDtypeStruct(shape, jnp.float32)
        hbm = pl.BlockSpec(memory_space=pltpu.HBM)
        high, low = halves(forward)
        table = np.concatenate([high, low], axis=1)
        sent = pl.pallas_call(
            lambda *refs: rows_to_slots(n, *refs),
            out_shape=out(n.devices, n.pieces, n.height, LANES),
            in_specs=[hbm] * 3, out_specs=whole, name="rows_to_slots", compiler_params=GRANT,
            scratch_shapes=[
                pltpu.VMEM(dense.shape, jnp.float32), pltpu.VMEM(sparse.shape, jnp.float32),
                pltpu.VMEM((2 * n.rows, 2 * n.rows), jnp.bfloat16), pltpu.SemaphoreType.DMA((3,)),
            ],
        )(*(pltpu.with_memory_space_constraint(v, pltpu.HBM) for v in (dense, sparse, jnp.asarray(table))))
        taken = lax.all_to_all(sent, AXES, 0, 0, tiled=True)
        mixed = pl.pallas_call(
            lambda *refs: middle(n, *refs),
            out_shape=out(n.devices, 2 * n.tiles, n.nf, LANES),
            in_specs=[scalar] + [whole] * 7, out_specs=whole, name="middle", compiler_params=GRANT,
            scratch_shapes=[
                pltpu.VMEM((n.all_entries + n.all_blocks, n.nf, 2 * LANES), jnp.float32),
                pltpu.VMEM((n.all_entries + n.all_blocks + RUN, n.nf, 3 * LANES), jnp.float32),
            ],
        )(pattern, taken, jnp.asarray(phase, jnp.float32), jnp.asarray(twist, jnp.float32), *halves(dft), *halves(idft))
        back = lax.all_to_all(mixed, AXES, 0, 0, tiled=True)
        return pl.pallas_call(
            lambda *refs: slots_to_rows(n, *refs),
            out_shape=out(*dense.shape),
            in_specs=[whole] * 2, out_specs=hbm, name="slots_to_rows", compiler_params=GRANT,
            scratch_shapes=[pltpu.VMEM(dense.shape, jnp.float32), pltpu.SemaphoreType.DMA((min(8, n.tiles),))],
        )(back, np.concatenate(halves(backward), axis=1))

    return jax.shard_map(
        local,
        mesh=mesh,
        in_specs=(P(("groups", "blk"), "sub", None), P(("groups", "blk"), "sub", None), P("groups")),
        out_specs=P(("groups", "blk"), "sub", None),
        check_vma=False,
    )
```

```python
import math

import jax
import jax.numpy as jnp
import numpy as np
from jax import lax
from jax.experimental import pallas as pl
from jax.experimental.pallas import tpu as pltpu
from jax.sharding import PartitionSpec as P

LANES = 128
GRANT = pltpu.CompilerParams(vmem_limit_bytes=16 * 2**20)
AXES = ("blk", "sub")


def halves(table):
    table = np.asarray(table, np.float32)
    high = table.astype(jnp.bfloat16)
    low = (table - high.astype(np.float32)).astype(jnp.bfloat16)
    return high, low


def split(values):
    high = values.astype(jnp.bfloat16)
    return high, (values - high.astype(jnp.float32)).astype(jnp.bfloat16)


def product3(left, right, dims):
    dot = lambda a, b: lax.dot_general(a, b, (dims, ((), ())), preferred_element_type=jnp.float32)
    return dot(left[0], right[0]) + (dot(left[0], right[1]) + dot(left[1], right[0]))


def regroup(tiles, width):
    count = len(tiles)
    group = lax.broadcasted_iota(jnp.int32, tiles[0].shape, len(tiles[0].shape) - 1) // width
    tiles = list(tiles)
    step = 1
    while step < count:
        keep = (group & step) == 0
        tiles = [jnp.where(keep, tiles[m], tiles[(m + step) % count]) for m in range(count)]
        step *= 2
    return [tiles[-j % count] for j in range(count)]


class Sizes:
    def __init__(self, dense, sparse, pattern, mesh_shape):
        self.z, self.subs = mesh_shape["blk"], mesh_shape["sub"]
        self.devices = self.z * self.subs
        self.blocks, self.q, self.rows = dense.shape
        self.entries = sparse.shape[0]
        self.all_entries = pattern.shape[0]
        self.nf = self.rows // self.devices
        self.tiles = self.blocks * self.q // LANES
        self.all_blocks = self.blocks * self.z
        self.parts = 2 if self.nf % 2 == 0 and 4 * self.entries * self.q <= LANES else 1
        self.height = self.nf // self.parts
        self.pieces = (2 * self.tiles) * self.parts + 1


def tables(n):
    f = np.arange(n.rows) + 0.5
    r = np.arange(n.rows)
    q = np.arange(LANES)
    arm = 2 * math.pi * f[:, None] * r[None, :] / (2 * n.rows)
    order = lambda c, s: np.stack([c.reshape(n.devices, n.nf, -1), s.reshape(n.devices, n.nf, -1)], 1).reshape(2 * n.rows, -1)
    forward = order(np.cos(arm), -np.sin(arm))
    backward = order(np.cos(arm), -np.sin(arm)) / (n.rows * LANES)
    twist = 2 * math.pi * f[:, None] * q[None, :] / (2 * n.rows * LANES)
    twist = np.stack([np.cos(twist), -np.sin(twist)], 0).reshape(2, n.devices, n.nf, LANES)
    turn = 2 * math.pi * (q[:, None] * q[None, :] % LANES) / LANES
    c, s = np.cos(turn), np.sin(turn)
    dft = np.block([[c, -s], [s, c]])
    idft = np.block([[c, s], [-s, c]])
    phase = 2 * math.pi * (np.arange(n.subs)[:, None] * q[None, :] % n.subs) / n.subs
    phase = np.stack([np.cos(phase), -np.sin(phase)], 0).reshape(2, n.subs, 1, LANES)
    return forward, backward, phase, twist, dft, idft


def rows_to_slots(n, dense_hbm, sparse_hbm, weights_hbm, out_ref, dense, sparse, weights, sems):
    nf = n.nf
    contract = ((1,), (1,))
    group = LANES // n.q
    width = n.entries * n.q
    loads = [
        pltpu.make_async_copy(weights_hbm, weights, sems.at[0]),
        pltpu.make_async_copy(sparse_hbm, sparse, sems.at[1]),
        pltpu.make_async_copy(dense_hbm, dense, sems.at[2]),
    ]
    for load in loads:
        load.start()
    for load in loads:
        load.wait()
    first, second = weights[:, :n.rows], weights[:, n.rows:]
    twice = jnp.concatenate([first, first], axis=1)
    me = lax.axis_index("sub")

    def slots_of(rows):
        high, low = split(rows)
        both = jnp.concatenate([high, low], axis=1)
        dot = lambda x, y: lax.dot_general(x, y, (contract, ((), ())), preferred_element_type=jnp.float32)
        return dot(twice, both) + dot(second, high)

    few = slots_of(sparse[...].reshape(width, n.rows))
    for d in range(n.devices):
        pieces = []
        for p in range(n.parts):
            for c in range(2):
                at = (d * 2 + c) * nf + p * n.height
                pieces.append(few[at:at + n.height])
        if 2 * n.parts * width < LANES:
            pieces.append(jnp.zeros((n.height, LANES - 2 * n.parts * width), jnp.float32))
        out_ref[d, n.pieces - 1] = jnp.concatenate(pieces, axis=1)
    rows = [dense[t * group + lax.rem(g - me + group, group)] for t in range(n.tiles) for g in range(group)]
    slots = slots_of(jnp.concatenate(rows, axis=0))
    for t in range(n.tiles):
        for d in range(n.devices):
            for c in range(2):
                at = (d * 2 + c) * nf
                tile = slots[at:at + nf, t * LANES:(t + 1) * LANES]
                first_piece = (c * n.tiles + t) * n.parts
                out_ref[d, first_piece:first_piece + n.parts] = tile.reshape(n.parts, n.height, LANES)


RUN = 8


def middle(n, pattern_ref, in_ref, phase_ref, twist_ref, dft_h, dft_l, idft_h, idft_l, out_ref, wave, spec):
    nf = n.nf
    me = lax.axis_index("blk") * n.subs + lax.axis_index("sub")
    group = n.subs
    turned = [[twist_ref[c, me] if j == 0 else pltpu.roll(twist_ref[c, me], j * n.q, 1) for c in range(2)] for j in range(group)]
    contract = ((1,), (0,))
    base = n.all_entries
    width = n.entries * n.q

    def store(index, re, im, j=0):
        tc, ts = turned[j]
        wave[index, :, :LANES] = re * tc - im * ts
        wave[index, :, LANES:] = re * ts + im * tc

    def transform(at, count, table):
        rows = wave[at:at + count].reshape(count * nf, 2 * LANES)
        return product3(split(rows), table, contract).reshape(count, nf, 2 * LANES)

    def tile(source, i):
        return in_ref[source, i * n.parts:(i + 1) * n.parts].reshape(nf, LANES)

    def gather(z):
        if z == 0:
            for y in range(n.z):
                few = [in_ref[y * n.subs + s, n.pieces - 1] for s in range(group)]
                for e in range(n.entries):
                    re, im = (
                        jnp.concatenate([
                            jnp.concatenate([
                                v[:, (p * 2 + c) * width + e * n.q:(p * 2 + c) * width + (e + 1) * n.q]
                                for v in few], axis=1)
                            for p in range(n.parts)], axis=0)
                        for c in range(2))
                    store(y * n.entries + e, re, im)
        for t in range(n.tiles):
            re = regroup([tile(z * n.subs + s, t) for s in range(group)], n.q)
            im = regroup([tile(z * n.subs + s, n.tiles + t) for s in range(group)], n.q)
            for j in range(group):
                store(base + z * n.blocks + t * group + j, re[j], im[j], j)

    def forward(z):
        at = base + z * n.blocks if z else 0
        count = n.blocks if z else base + n.blocks
        result = transform(at, count, (dft_h[...], dft_l[...]))
        re, im = result[:, :, :LANES], result[:, :, LANES:]
        spec[at:at + count, :, :LANES] = re
        spec[at:at + count, :, LANES:2 * LANES] = im
        spec[at:at + count, :, 2 * LANES:] = re + im

    gather(0)
    for z in range(1, n.z):
        gather(z)
        forward(z - 1)
    forward(n.z - 1)
    spec[base + n.all_blocks:base + n.all_blocks + RUN] = spec[base:base + RUN]

    shifts = [lax.rem(pattern_ref[e], n.all_blocks) for e in range(n.all_entries)]
    slot = lax.broadcasted_iota(jnp.int32, (nf, LANES), 0) + me * nf
    sign = jnp.where(lax.rem(slot, 2) == 0, 1.0, -1.0).astype(jnp.float32)
    over_re, over_im = -sign * phase_ref[1, 1], sign * phase_ref[0, 1]

    def factors():
        out = []
        for e in range(n.all_entries):
            xr, xi = spec[e, :, :LANES], spec[e, :, LANES:2 * LANES]
            power = lax.rem(shifts[e], group)
            pr, pi = phase_ref[0, power], phase_ref[1, power]
            sr, si = xr * pr - xi * pi, xr * pi + xi * pr
            out.append((sr, si + sr, si - sr))
        return out

    def starts(k):
        out = []
        for shift in shifts:
            j = k - shift
            out.append(base + jnp.where(j < 0, j + n.all_blocks, j))
        return out

    def convolved(rows, i, table):
        t = u = v = None
        for e, (sr, ssum, sdiff) in enumerate(table):
            at = rows[e] + i
            a = spec[at, :, 2 * LANES:] * sr
            b = spec[at, :, LANES:2 * LANES] * ssum
            c = spec[at, :, :LANES] * sdiff
            t, u, v = (a, b, c) if t is None else (t + a, u + b, v + c)
        return t - u, t + v

    def run_of(k, before, table):
        rows = starts(k)
        for i in range(RUN):
            re, im = convolved(rows, i, table)
            wave[k + i, :, :LANES] = re + (over_re * before[0] - over_im * before[1])
            wave[k + i, :, LANES:] = im + (over_re * before[1] + over_im * before[0])
            before = (re, im)
        return before

    def convolve(z, before):
        if n.all_blocks * n.all_entries <= 1024:
            table = factors()
            for k in range(z * n.blocks, (z + 1) * n.blocks, RUN):
                before = run_of(k, before, table)
            return before
        return lax.fori_loop(
            0, n.blocks // RUN,
            lambda i, carry: run_of(z * n.blocks + i * RUN, carry, factors()), before)

    def scatter(z):
        result = transform(z * n.blocks, n.blocks, (idft_h[...], idft_l[...]))
        for t in range(n.tiles):
            re, im = [], []
            for j in range(group):
                tc, ts = turned[j]
                er, ei = result[t * group + j, :, :LANES], result[t * group + j, :, LANES:]
                re.append(er * tc + ei * ts)
                im.append(ei * tc - er * ts)
            for s, value in enumerate(regroup(re, n.q)):
                out_ref[z * n.subs + s, t] = value
            for s, value in enumerate(regroup(im, n.q)):
                out_ref[z * n.subs + s, n.tiles + t] = value

    before = convolved(starts(n.all_blocks - 1), 0, factors())
    before = convolve(0, before)
    for z in range(1, n.z):
        before = convolve(z, before)
        scatter(z - 1)
    scatter(n.z - 1)


def slots_to_rows(n, in_ref, weights_ref, out_hbm, rows_ref, sems):
    both = weights_ref[...]
    group = LANES // n.q
    me = lax.axis_index("sub")
    steps = min(4, n.tiles)
    per = n.tiles // steps
    dot = lambda a, b: lax.dot_general(a, b, (((1,), (0,)), ((), ())), preferred_element_type=jnp.float32)
    stores = []
    for s in range(steps):
        columns = []
        for t in range(s * per, (s + 1) * per):
            pieces = [in_ref[d, c * n.tiles + t] for d in range(n.devices) for c in range(2)]
            columns.append(jnp.concatenate(pieces, axis=0))
        high, low = split(jnp.concatenate(columns, axis=1))
        wide = dot(both, high)
        rows = wide[:n.rows] + (wide[n.rows:] + dot(both[:n.rows], low))
        rows = jnp.transpose(rows)
        for i in range(per):
            for g in range(group):
                at = i * LANES + g * n.q
                rows_ref[(s * per + i) * group + lax.rem(g - me + group, group)] = rows[at:at + n.q]
        part = pl.ds(s * per * group, per * group)
        stores.append(pltpu.make_async_copy(rows_ref.at[part], out_hbm.at[part], sems.at[s]))
        stores[-1].start()
    for store in stores:
        store.wait()


def solution(mesh):
    def local(dense, sparse, pattern):
        n = Sizes(dense, sparse, pattern, mesh.shape)
        forward, backward, phase, twist, dft, idft = tables(n)
        scalar = pl.BlockSpec(memory_space=pltpu.SMEM)
        whole = pl.BlockSpec(memory_space=pltpu.VMEM)
        out = lambda *shape: jax.ShapeDtypeStruct(shape, jnp.float32)
        hbm = pl.BlockSpec(memory_space=pltpu.HBM)
        high, low = halves(forward)
        table = np.concatenate([high, low], axis=1)
        sent = pl.pallas_call(
            lambda *refs: rows_to_slots(n, *refs),
            out_shape=out(n.devices, n.pieces, n.height, LANES),
            in_specs=[hbm] * 3, out_specs=whole, name="rows_to_slots", compiler_params=GRANT,
            scratch_shapes=[
                pltpu.VMEM(dense.shape, jnp.float32), pltpu.VMEM(sparse.shape, jnp.float32),
                pltpu.VMEM((2 * n.rows, 2 * n.rows), jnp.bfloat16), pltpu.SemaphoreType.DMA((3,)),
            ],
        )(*(pltpu.with_memory_space_constraint(v, pltpu.HBM) for v in (dense, sparse, jnp.asarray(table))))
        taken = lax.all_to_all(sent, AXES, 0, 0, tiled=True)
        mixed = pl.pallas_call(
            lambda *refs: middle(n, *refs),
            out_shape=out(n.devices, 2 * n.tiles, n.nf, LANES),
            in_specs=[scalar] + [whole] * 7, out_specs=whole, name="middle", compiler_params=GRANT,
            scratch_shapes=[
                pltpu.VMEM((n.all_entries + n.all_blocks, n.nf, 2 * LANES), jnp.float32),
                pltpu.VMEM((n.all_entries + n.all_blocks + RUN, n.nf, 3 * LANES), jnp.float32),
            ],
        )(pattern, taken, jnp.asarray(phase, jnp.float32), jnp.asarray(twist, jnp.float32), *halves(dft), *halves(idft))
        back = lax.all_to_all(mixed, AXES, 0, 0, tiled=True)
        return pl.pallas_call(
            lambda *refs: slots_to_rows(n, *refs),
            out_shape=out(*dense.shape),
            in_specs=[whole] * 2, out_specs=hbm, name="slots_to_rows", compiler_params=GRANT,
            scratch_shapes=[pltpu.VMEM(dense.shape, jnp.float32), pltpu.SemaphoreType.DMA((min(4, n.tiles),))],
        )(back, np.concatenate(halves(backward.T), axis=0))

    return jax.shard_map(
        local,
        mesh=mesh,
        in_specs=(P(("groups", "blk"), "sub", None), P(("groups", "blk"), "sub", None), P("groups")),
        out_specs=P(("groups", "blk"), "sub", None),
        check_vma=False,
    )
```

```python
import math

import jax
import jax.numpy as jnp
import numpy as np
from jax import lax
from jax.experimental import pallas as pl
from jax.experimental.pallas import tpu as pltpu
from jax.sharding import PartitionSpec as P

LANES = 128
GRANT = pltpu.CompilerParams(vmem_limit_bytes=16 * 2**20)
AXES = ("blk", "sub")


def halves(table):
    table = np.asarray(table, np.float32)
    high = table.astype(jnp.bfloat16)
    low = (table - high.astype(np.float32)).astype(jnp.bfloat16)
    return high, low


def split(values):
    high = values.astype(jnp.bfloat16)
    return high, (values - high.astype(jnp.float32)).astype(jnp.bfloat16)


def product3(left, right, dims):
    dot = lambda a, b: lax.dot_general(a, b, (dims, ((), ())), preferred_element_type=jnp.float32)
    return dot(left[0], right[0]) + (dot(left[0], right[1]) + dot(left[1], right[0]))


def regroup(tiles, width):
    count = len(tiles)
    group = lax.broadcasted_iota(jnp.int32, tiles[0].shape, len(tiles[0].shape) - 1) // width
    tiles = list(tiles)
    step = 1
    while step < count:
        keep = (group & step) == 0
        tiles = [jnp.where(keep, tiles[m], tiles[(m + step) % count]) for m in range(count)]
        step *= 2
    return [tiles[-j % count] for j in range(count)]


class Sizes:
    def __init__(self, dense, sparse, pattern, mesh_shape):
        self.z, self.subs = mesh_shape["blk"], mesh_shape["sub"]
        self.devices = self.z * self.subs
        self.blocks, self.q, self.rows = dense.shape
        self.entries = sparse.shape[0]
        self.all_entries = pattern.shape[0]
        self.nf = self.rows // self.devices
        self.tiles = self.blocks * self.q // LANES
        self.all_blocks = self.blocks * self.z
        self.parts = 2 if self.nf % 2 == 0 and 4 * self.entries * self.q <= LANES else 1
        self.height = self.nf // self.parts
        self.pieces = (2 * self.tiles) * self.parts + 1


def tables(n):
    f = np.arange(n.rows) + 0.5
    r = np.arange(n.rows)
    q = np.arange(LANES)
    arm = 2 * math.pi * f[:, None] * r[None, :] / (2 * n.rows)
    order = lambda c, s: np.stack([c.reshape(n.devices, n.nf, -1), s.reshape(n.devices, n.nf, -1)], 1).reshape(2 * n.rows, -1)
    forward = order(np.cos(arm), -np.sin(arm))
    backward = order(np.cos(arm), -np.sin(arm)) / (n.rows * LANES)
    twist = 2 * math.pi * f[:, None] * q[None, :] / (2 * n.rows * LANES)
    twist = np.stack([np.cos(twist), -np.sin(twist)], 0).reshape(2, n.devices, n.nf, LANES)
    turn = 2 * math.pi * (q[:, None] * q[None, :] % LANES) / LANES
    c, s = np.cos(turn), np.sin(turn)
    dft = np.block([[c, -s], [s, c]])
    idft = np.block([[c, s], [-s, c]])
    phase = 2 * math.pi * (np.arange(n.subs)[:, None] * q[None, :] % n.subs) / n.subs
    phase = np.stack([np.cos(phase), -np.sin(phase)], 0).reshape(2, n.subs, 1, LANES)
    return forward, backward, phase, twist, dft, idft


def rows_to_slots(n, dense_hbm, sparse_hbm, weights_hbm, out_ref, dense, sparse, weights, sems):
    nf = n.nf
    contract = ((1,), (1,))
    group = LANES // n.q
    width = n.entries * n.q
    loads = [
        pltpu.make_async_copy(weights_hbm, weights, sems.at[0]),
        pltpu.make_async_copy(sparse_hbm, sparse, sems.at[1]),
        pltpu.make_async_copy(dense_hbm, dense, sems.at[2]),
    ]
    for load in reversed(loads):
        load.start()
    for load in loads:
        load.wait()
    first, second = weights[:, :n.rows], weights[:, n.rows:]
    twice = jnp.concatenate([first, first], axis=1)
    me = lax.axis_index("sub")

    def slots_of(rows):
        high, low = split(rows)
        both = jnp.concatenate([high, low], axis=1)
        dot = lambda x, y: lax.dot_general(x, y, (contract, ((), ())), preferred_element_type=jnp.float32)
        return dot(twice, both) + dot(second, high)

    few = slots_of(sparse[...].reshape(width, n.rows))
    for d in range(n.devices):
        pieces = []
        for p in range(n.parts):
            for c in range(2):
                at = (d * 2 + c) * nf + p * n.height
                pieces.append(few[at:at + n.height])
        if 2 * n.parts * width < LANES:
            pieces.append(jnp.zeros((n.height, LANES - 2 * n.parts * width), jnp.float32))
        out_ref[d, n.pieces - 1] = jnp.concatenate(pieces, axis=1)
    rows = [dense[t * group + lax.rem(g - me + group, group)] for t in range(n.tiles) for g in range(group)]
    slots = slots_of(jnp.concatenate(rows, axis=0))
    for t in range(n.tiles):
        for d in range(n.devices):
            for c in range(2):
                at = (d * 2 + c) * nf
                tile = slots[at:at + nf, t * LANES:(t + 1) * LANES]
                first_piece = (c * n.tiles + t) * n.parts
                out_ref[d, first_piece:first_piece + n.parts] = tile.reshape(n.parts, n.height, LANES)


RUN = 8


def middle(n, pattern_ref, in_ref, phase_ref, twist_ref, dft_h, dft_l, idft_h, idft_l, out_ref, wave, spec):
    nf = n.nf
    me = lax.axis_index("blk") * n.subs + lax.axis_index("sub")
    group = n.subs
    turned = [[twist_ref[c, me] if j == 0 else pltpu.roll(twist_ref[c, me], j * n.q, 1) for c in range(2)] for j in range(group)]
    contract = ((1,), (0,))
    base = n.all_entries
    width = n.entries * n.q

    def store(index, re, im, j=0):
        tc, ts = turned[j]
        wave[index, :, :LANES] = re * tc - im * ts
        wave[index, :, LANES:] = re * ts + im * tc

    def transform(at, count, table):
        rows = wave[at:at + count].reshape(count * nf, 2 * LANES)
        return product3(split(rows), table, contract).reshape(count, nf, 2 * LANES)

    def tile(source, i):
        return in_ref[source, i * n.parts:(i + 1) * n.parts].reshape(nf, LANES)

    def gather(z):
        if z == 0:
            for y in range(n.z):
                few = [in_ref[y * n.subs + s, n.pieces - 1] for s in range(group)]
                for e in range(n.entries):
                    re, im = (
                        jnp.concatenate([
                            jnp.concatenate([
                                v[:, (p * 2 + c) * width + e * n.q:(p * 2 + c) * width + (e + 1) * n.q]
                                for v in few], axis=1)
                            for p in range(n.parts)], axis=0)
                        for c in range(2))
                    store(y * n.entries + e, re, im)
        for t in range(n.tiles):
            re = regroup([tile(z * n.subs + s, t) for s in range(group)], n.q)
            im = regroup([tile(z * n.subs + s, n.tiles + t) for s in range(group)], n.q)
            for j in range(group):
                store(base + z * n.blocks + t * group + j, re[j], im[j], j)

    def forward(z):
        at = base + z * n.blocks if z else 0
        count = n.blocks if z else base + n.blocks
        result = transform(at, count, (dft_h[...], dft_l[...]))
        re, im = result[:, :, :LANES], result[:, :, LANES:]
        spec[at:at + count, :, :LANES] = re
        spec[at:at + count, :, LANES:2 * LANES] = im
        spec[at:at + count, :, 2 * LANES:] = re + im

    gather(0)
    for z in range(1, n.z):
        gather(z)
        forward(z - 1)
    forward(n.z - 1)
    spec[base + n.all_blocks:base + n.all_blocks + RUN] = spec[base:base + RUN]

    shifts = [lax.rem(pattern_ref[e], n.all_blocks) for e in range(n.all_entries)]
    slot = lax.broadcasted_iota(jnp.int32, (nf, LANES), 0) + me * nf
    sign = jnp.where(lax.rem(slot, 2) == 0, 1.0, -1.0).astype(jnp.float32)
    over_re, over_im = -sign * phase_ref[1, 1], sign * phase_ref[0, 1]

    def factors():
        out = []
        for e in range(n.all_entries):
            xr, xi = spec[e, :, :LANES], spec[e, :, LANES:2 * LANES]
            power = lax.rem(shifts[e], group)
            pr, pi = phase_ref[0, power], phase_ref[1, power]
            sr, si = xr * pr - xi * pi, xr * pi + xi * pr
            out.append((sr, si + sr, si - sr))
        return out

    def starts(k):
        out = []
        for shift in shifts:
            j = k - shift
            out.append(base + jnp.where(j < 0, j + n.all_blocks, j))
        return out

    def convolved(rows, i, table):
        t = u = v = None
        for e, (sr, ssum, sdiff) in enumerate(table):
            at = rows[e] + i
            a = spec[at, :, 2 * LANES:] * sr
            b = spec[at, :, LANES:2 * LANES] * ssum
            c = spec[at, :, :LANES] * sdiff
            t, u, v = (a, b, c) if t is None else (t + a, u + b, v + c)
        return t - u, t + v

    def run_of(k, before, table):
        rows = starts(k)
        for i in range(RUN):
            re, im = convolved(rows, i, table)
            wave[k + i, :, :LANES] = re + (over_re * before[0] - over_im * before[1])
            wave[k + i, :, LANES:] = im + (over_re * before[1] + over_im * before[0])
            before = (re, im)
        return before

    def convolve(z, before):
        if n.all_blocks * n.all_entries <= 1024:
            table = factors()
            for k in range(z * n.blocks, (z + 1) * n.blocks, RUN):
                before = run_of(k, before, table)
            return before
        return lax.fori_loop(
            0, n.blocks // RUN,
            lambda i, carry: run_of(z * n.blocks + i * RUN, carry, factors()), before)

    def scatter(z):
        result = transform(z * n.blocks, n.blocks, (idft_h[...], idft_l[...]))
        for t in range(n.tiles):
            re, im = [], []
            for j in range(group):
                tc, ts = turned[j]
                er, ei = result[t * group + j, :, :LANES], result[t * group + j, :, LANES:]
                re.append(er * tc + ei * ts)
                im.append(ei * tc - er * ts)
            for s, value in enumerate(regroup(re, n.q)):
                out_ref[z * n.subs + s, t] = value
            for s, value in enumerate(regroup(im, n.q)):
                out_ref[z * n.subs + s, n.tiles + t] = value

    before = convolved(starts(n.all_blocks - 1), 0, factors())
    before = convolve(0, before)
    for z in range(1, n.z):
        before = convolve(z, before)
        scatter(z - 1)
    scatter(n.z - 1)


def slots_to_rows(n, in_ref, weights_ref, out_hbm, rows_ref, sems):
    both = weights_ref[...]
    first = both[:, :n.rows]
    group = LANES // n.q
    me = lax.axis_index("sub")
    steps = min(8, n.tiles)
    per = n.tiles // steps
    dot = lambda a, b: lax.dot_general(a, b, (((0,), (0,)), ((), ())), preferred_element_type=jnp.float32)
    stores = []
    for s in range(steps):
        for t in range(s * per, (s + 1) * per):
            pieces = [in_ref[d, c * n.tiles + t] for d in range(n.devices) for c in range(2)]
            high, low = split(jnp.concatenate(pieces, axis=0))
            wide = dot(high, both)
            rows = wide[:, :n.rows] + (wide[:, n.rows:] + dot(low, first))
            for g in range(group):
                rows_ref[t * group + lax.rem(g - me + group, group)] = rows[g * n.q:(g + 1) * n.q]
        part = pl.ds(s * per * group, per * group)
        stores.append(pltpu.make_async_copy(rows_ref.at[part], out_hbm.at[part], sems.at[s]))
        stores[-1].start()
    for store in stores:
        store.wait()


def solution(mesh):
    def local(dense, sparse, pattern):
        n = Sizes(dense, sparse, pattern, mesh.shape)
        forward, backward, phase, twist, dft, idft = tables(n)
        scalar = pl.BlockSpec(memory_space=pltpu.SMEM)
        whole = pl.BlockSpec(memory_space=pltpu.VMEM)
        out = lambda *shape: jax.ShapeDtypeStruct(shape, jnp.float32)
        hbm = pl.BlockSpec(memory_space=pltpu.HBM)
        high, low = halves(forward)
        table = np.concatenate([high, low], axis=1)
        sent = pl.pallas_call(
            lambda *refs: rows_to_slots(n, *refs),
            out_shape=out(n.devices, n.pieces, n.height, LANES),
            in_specs=[hbm] * 3, out_specs=whole, name="rows_to_slots", compiler_params=GRANT,
            scratch_shapes=[
                pltpu.VMEM(dense.shape, jnp.float32), pltpu.VMEM(sparse.shape, jnp.float32),
                pltpu.VMEM((2 * n.rows, 2 * n.rows), jnp.bfloat16), pltpu.SemaphoreType.DMA((3,)),
            ],
        )(*(pltpu.with_memory_space_constraint(v, pltpu.HBM) for v in (dense, sparse, jnp.asarray(table))))
        taken = lax.all_to_all(sent, AXES, 0, 0, tiled=True)
        mixed = pl.pallas_call(
            lambda *refs: middle(n, *refs),
            out_shape=out(n.devices, 2 * n.tiles, n.nf, LANES),
            in_specs=[scalar] + [whole] * 7, out_specs=whole, name="middle", compiler_params=GRANT,
            scratch_shapes=[
                pltpu.VMEM((n.all_entries + n.all_blocks, n.nf, 2 * LANES), jnp.float32),
                pltpu.VMEM((n.all_entries + n.all_blocks + RUN, n.nf, 3 * LANES), jnp.float32),
            ],
        )(pattern, taken, jnp.asarray(phase, jnp.float32), jnp.asarray(twist, jnp.float32), *halves(dft), *halves(idft))
        back = lax.all_to_all(mixed, AXES, 0, 0, tiled=True)
        return pl.pallas_call(
            lambda *refs: slots_to_rows(n, *refs),
            out_shape=out(*dense.shape),
            in_specs=[whole] * 2, out_specs=hbm, name="slots_to_rows", compiler_params=GRANT,
            scratch_shapes=[pltpu.VMEM(dense.shape, jnp.float32), pltpu.SemaphoreType.DMA((min(8, n.tiles),))],
        )(back, np.concatenate(halves(backward), axis=1))

    return jax.shard_map(
        local,
        mesh=mesh,
        in_specs=(P(("groups", "blk"), "sub", None), P(("groups", "blk"), "sub", None), P("groups")),
        out_specs=P(("groups", "blk"), "sub", None),
        check_vma=False,
    )
```

```python
import math

import jax
import jax.numpy as jnp
import numpy as np
from jax import lax
from jax.experimental import pallas as pl
from jax.experimental.pallas import tpu as pltpu
from jax.sharding import PartitionSpec as P

LANES = 128
GRANT = pltpu.CompilerParams(vmem_limit_bytes=16 * 2**20)
AXES = ("blk", "sub")


def halves(table):
    table = np.asarray(table, np.float32)
    high = table.astype(jnp.bfloat16)
    low = (table - high.astype(np.float32)).astype(jnp.bfloat16)
    return high, low


def split(values):
    high = values.astype(jnp.bfloat16)
    return high, (values - high.astype(jnp.float32)).astype(jnp.bfloat16)


def product3(left, right, dims):
    dot = lambda a, b: lax.dot_general(a, b, (dims, ((), ())), preferred_element_type=jnp.float32)
    return dot(left[0], right[0]) + (dot(left[0], right[1]) + dot(left[1], right[0]))


def regroup(tiles, width):
    count = len(tiles)
    group = lax.broadcasted_iota(jnp.int32, tiles[0].shape, len(tiles[0].shape) - 1) // width
    tiles = list(tiles)
    step = 1
    while step < count:
        keep = (group & step) == 0
        tiles = [jnp.where(keep, tiles[m], tiles[(m + step) % count]) for m in range(count)]
        step *= 2
    return [tiles[-j % count] for j in range(count)]


class Sizes:
    def __init__(self, dense, sparse, pattern, mesh_shape):
        self.z, self.subs = mesh_shape["blk"], mesh_shape["sub"]
        self.devices = self.z * self.subs
        self.blocks, self.q, self.rows = dense.shape
        self.entries = sparse.shape[0]
        self.all_entries = pattern.shape[0]
        self.nf = self.rows // self.devices
        self.tiles = self.blocks * self.q // LANES
        self.all_blocks = self.blocks * self.z
        self.parts = 2 if self.nf % 2 == 0 and 4 * self.entries * self.q <= LANES else 1
        self.height = self.nf // self.parts
        self.pieces = (2 * self.tiles) * self.parts + 1


def tables(n):
    f = np.arange(n.rows) + 0.5
    r = np.arange(n.rows)
    q = np.arange(LANES)
    arm = 2 * math.pi * f[:, None] * r[None, :] / (2 * n.rows)
    order = lambda c, s: np.stack([c.reshape(n.devices, n.nf, -1), s.reshape(n.devices, n.nf, -1)], 1).reshape(2 * n.rows, -1)
    forward = order(np.cos(arm), -np.sin(arm))
    backward = order(np.cos(arm), -np.sin(arm)) / (n.rows * LANES)
    twist = 2 * math.pi * f[:, None] * q[None, :] / (2 * n.rows * LANES)
    twist = np.stack([np.cos(twist), -np.sin(twist)], 0).reshape(2, n.devices, n.nf, LANES)
    turn = 2 * math.pi * (q[:, None] * q[None, :] % LANES) / LANES
    c, s = np.cos(turn), np.sin(turn)
    dft = np.block([[c, -s], [s, c]])
    idft = np.block([[c, s], [-s, c]])
    phase = 2 * math.pi * (np.arange(n.subs)[:, None] * q[None, :] % n.subs) / n.subs
    phase = np.stack([np.cos(phase), -np.sin(phase)], 0).reshape(2, n.subs, 1, LANES)
    return forward, backward, phase, twist, dft, idft


def rows_to_slots(n, dense_hbm, sparse_hbm, weights_hbm, out_ref, dense, sparse, weights, sems):
    nf = n.nf
    contract = ((1,), (1,))
    group = LANES // n.q
    width = n.entries * n.q
    loads = [
        pltpu.make_async_copy(weights_hbm, weights, sems.at[0]),
        pltpu.make_async_copy(sparse_hbm, sparse, sems.at[1]),
        pltpu.make_async_copy(dense_hbm.at[pl.ds(0, n.blocks // 2)], dense.at[pl.ds(0, n.blocks // 2)], sems.at[2]),
        pltpu.make_async_copy(dense_hbm.at[pl.ds(n.blocks // 2, n.blocks - n.blocks // 2)], dense.at[pl.ds(n.blocks // 2, n.blocks - n.blocks // 2)], sems.at[3]),
    ]
    for load in reversed(loads):
        load.start()
    for load in loads:
        load.wait()
    first, second = weights[:, :n.rows], weights[:, n.rows:]
    twice = jnp.concatenate([first, first], axis=1)
    me = lax.axis_index("sub")

    def slots_of(rows):
        high, low = split(rows)
        both = jnp.concatenate([high, low], axis=1)
        dot = lambda x, y: lax.dot_general(x, y, (contract, ((), ())), preferred_element_type=jnp.float32)
        return dot(twice, both) + dot(second, high)

    few = slots_of(sparse[...].reshape(width, n.rows))
    for d in range(n.devices):
        pieces = []
        for p in range(n.parts):
            for c in range(2):
                at = (d * 2 + c) * nf + p * n.height
                pieces.append(few[at:at + n.height])
        if 2 * n.parts * width < LANES:
            pieces.append(jnp.zeros((n.height, LANES - 2 * n.parts * width), jnp.float32))
        out_ref[d, n.pieces - 1] = jnp.concatenate(pieces, axis=1)
    rows = [dense[t * group + lax.rem(g - me + group, group)] for t in range(n.tiles) for g in range(group)]
    slots = slots_of(jnp.concatenate(rows, axis=0))
    for t in range(n.tiles):
        for d in range(n.devices):
            for c in range(2):
                at = (d * 2 + c) * nf
                tile = slots[at:at + nf, t * LANES:(t + 1) * LANES]
                first_piece = (c * n.tiles + t) * n.parts
                out_ref[d, first_piece:first_piece + n.parts] = tile.reshape(n.parts, n.height, LANES)


RUN = 8


def middle(n, pattern_ref, in_ref, phase_ref, twist_ref, dft_h, dft_l, idft_h, idft_l, out_ref, wave, spec):
    nf = n.nf
    me = lax.axis_index("blk") * n.subs + lax.axis_index("sub")
    group = n.subs
    turned = [[twist_ref[c, me] if j == 0 else pltpu.roll(twist_ref[c, me], j * n.q, 1) for c in range(2)] for j in range(group)]
    contract = ((1,), (0,))
    base = n.all_entries
    width = n.entries * n.q

    def store(index, re, im, j=0):
        tc, ts = turned[j]
        wave[index, :, :LANES] = re * tc - im * ts
        wave[index, :, LANES:] = re * ts + im * tc

    def transform(at, count, table):
        rows = wave[at:at + count].reshape(count * nf, 2 * LANES)
        return product3(split(rows), table, contract).reshape(count, nf, 2 * LANES)

    def tile(source, i):
        return in_ref[source, i * n.parts:(i + 1) * n.parts].reshape(nf, LANES)

    def gather(z):
        if z == 0:
            for y in range(n.z):
                few = [in_ref[y * n.subs + s, n.pieces - 1] for s in range(group)]
                for e in range(n.entries):
                    re, im = (
                        jnp.concatenate([
                            jnp.concatenate([
                                v[:, (p * 2 + c) * width + e * n.q:(p * 2 + c) * width + (e + 1) * n.q]
                                for v in few], axis=1)
                            for p in range(n.parts)], axis=0)
                        for c in range(2))
                    store(y * n.entries + e, re, im)
        for t in range(n.tiles):
            re = regroup([tile(z * n.subs + s, t) for s in range(group)], n.q)
            im = regroup([tile(z * n.subs + s, n.tiles + t) for s in range(group)], n.q)
            for j in range(group):
                store(base + z * n.blocks + t * group + j, re[j], im[j], j)

    def forward(z):
        at = base + z * n.blocks if z else 0
        count = n.blocks if z else base + n.blocks
        result = transform(at, count, (dft_h[...], dft_l[...]))
        re, im = result[:, :, :LANES], result[:, :, LANES:]
        spec[at:at + count, :, :LANES] = re
        spec[at:at + count, :, LANES:2 * LANES] = im
        spec[at:at + count, :, 2 * LANES:] = re + im

    gather(0)
    for z in range(1, n.z):
        gather(z)
        forward(z - 1)
    forward(n.z - 1)
    spec[base + n.all_blocks:base + n.all_blocks + RUN] = spec[base:base + RUN]

    shifts = [lax.rem(pattern_ref[e], n.all_blocks) for e in range(n.all_entries)]
    slot = lax.broadcasted_iota(jnp.int32, (nf, LANES), 0) + me * nf
    sign = jnp.where(lax.rem(slot, 2) == 0, 1.0, -1.0).astype(jnp.float32)
    over_re, over_im = -sign * phase_ref[1, 1], sign * phase_ref[0, 1]

    def factors():
        out = []
        for e in range(n.all_entries):
            xr, xi = spec[e, :, :LANES], spec[e, :, LANES:2 * LANES]
            power = lax.rem(shifts[e], group)
            pr, pi = phase_ref[0, power], phase_ref[1, power]
            sr, si = xr * pr - xi * pi, xr * pi + xi * pr
            out.append((sr, si + sr, si - sr))
        return out

    def starts(k):
        out = []
        for shift in shifts:
            j = k - shift
            out.append(base + jnp.where(j < 0, j + n.all_blocks, j))
        return out

    def convolved(rows, i, table):
        t = u = v = None
        for e, (sr, ssum, sdiff) in enumerate(table):
            at = rows[e] + i
            a = spec[at, :, 2 * LANES:] * sr
            b = spec[at, :, LANES:2 * LANES] * ssum
            c = spec[at, :, :LANES] * sdiff
            t, u, v = (a, b, c) if t is None else (t + a, u + b, v + c)
        return t - u, t + v

    def run_of(k, before, table):
        rows = starts(k)
        for i in range(RUN):
            re, im = convolved(rows, i, table)
            wave[k + i, :, :LANES] = re + (over_re * before[0] - over_im * before[1])
            wave[k + i, :, LANES:] = im + (over_re * before[1] + over_im * before[0])
            before = (re, im)
        return before

    def convolve(z, before):
        if n.all_blocks * n.all_entries <= 1024:
            table = factors()
            for k in range(z * n.blocks, (z + 1) * n.blocks, RUN):
                before = run_of(k, before, table)
            return before
        return lax.fori_loop(
            0, n.blocks // RUN,
            lambda i, carry: run_of(z * n.blocks + i * RUN, carry, factors()), before)

    def scatter(z):
        result = transform(z * n.blocks, n.blocks, (idft_h[...], idft_l[...]))
        for t in range(n.tiles):
            re, im = [], []
            for j in range(group):
                tc, ts = turned[j]
                er, ei = result[t * group + j, :, :LANES], result[t * group + j, :, LANES:]
                re.append(er * tc + ei * ts)
                im.append(ei * tc - er * ts)
            for s, value in enumerate(regroup(re, n.q)):
                out_ref[z * n.subs + s, t] = value
            for s, value in enumerate(regroup(im, n.q)):
                out_ref[z * n.subs + s, n.tiles + t] = value

    before = convolved(starts(n.all_blocks - 1), 0, factors())
    before = convolve(0, before)
    for z in range(1, n.z):
        before = convolve(z, before)
        scatter(z - 1)
    scatter(n.z - 1)


def slots_to_rows(n, in_ref, weights_ref, out_hbm, rows_ref, sems):
    both = weights_ref[...]
    first = both[:, :n.rows]
    group = LANES // n.q
    me = lax.axis_index("sub")
    steps = min(8, n.tiles)
    per = n.tiles // steps
    dot = lambda a, b: lax.dot_general(a, b, (((0,), (0,)), ((), ())), preferred_element_type=jnp.float32)
    stores = []
    for s in range(steps):
        for t in range(s * per, (s + 1) * per):
            pieces = [in_ref[d, c * n.tiles + t] for d in range(n.devices) for c in range(2)]
            high, low = split(jnp.concatenate(pieces, axis=0))
            wide = dot(high, both)
            rows = wide[:, :n.rows] + (wide[:, n.rows:] + dot(low, first))
            for g in range(group):
                rows_ref[t * group + lax.rem(g - me + group, group)] = rows[g * n.q:(g + 1) * n.q]
        part = pl.ds(s * per * group, per * group)
        stores.append(pltpu.make_async_copy(rows_ref.at[part], out_hbm.at[part], sems.at[s]))
        stores[-1].start()
    for store in stores:
        store.wait()


def solution(mesh):
    def local(dense, sparse, pattern):
        n = Sizes(dense, sparse, pattern, mesh.shape)
        forward, backward, phase, twist, dft, idft = tables(n)
        scalar = pl.BlockSpec(memory_space=pltpu.SMEM)
        whole = pl.BlockSpec(memory_space=pltpu.VMEM)
        out = lambda *shape: jax.ShapeDtypeStruct(shape, jnp.float32)
        hbm = pl.BlockSpec(memory_space=pltpu.HBM)
        high, low = halves(forward)
        table = np.concatenate([high, low], axis=1)
        sent = pl.pallas_call(
            lambda *refs: rows_to_slots(n, *refs),
            out_shape=out(n.devices, n.pieces, n.height, LANES),
            in_specs=[hbm] * 3, out_specs=whole, name="rows_to_slots", compiler_params=GRANT,
            scratch_shapes=[
                pltpu.VMEM(dense.shape, jnp.float32), pltpu.VMEM(sparse.shape, jnp.float32),
                pltpu.VMEM((2 * n.rows, 2 * n.rows), jnp.bfloat16), pltpu.SemaphoreType.DMA((4,)),
            ],
        )(*(pltpu.with_memory_space_constraint(v, pltpu.HBM) for v in (dense, sparse, jnp.asarray(table))))
        taken = lax.all_to_all(sent, AXES, 0, 0, tiled=True)
        mixed = pl.pallas_call(
            lambda *refs: middle(n, *refs),
            out_shape=out(n.devices, 2 * n.tiles, n.nf, LANES),
            in_specs=[scalar] + [whole] * 7, out_specs=whole, name="middle", compiler_params=GRANT,
            scratch_shapes=[
                pltpu.VMEM((n.all_entries + n.all_blocks, n.nf, 2 * LANES), jnp.float32),
                pltpu.VMEM((n.all_entries + n.all_blocks + RUN, n.nf, 3 * LANES), jnp.float32),
            ],
        )(pattern, taken, jnp.asarray(phase, jnp.float32), jnp.asarray(twist, jnp.float32), *halves(dft), *halves(idft))
        back = lax.all_to_all(mixed, AXES, 0, 0, tiled=True)
        return pl.pallas_call(
            lambda *refs: slots_to_rows(n, *refs),
            out_shape=out(*dense.shape),
            in_specs=[whole] * 2, out_specs=hbm, name="slots_to_rows", compiler_params=GRANT,
            scratch_shapes=[pltpu.VMEM(dense.shape, jnp.float32), pltpu.SemaphoreType.DMA((min(8, n.tiles),))],
        )(back, np.concatenate(halves(backward), axis=1))

    return jax.shard_map(
        local,
        mesh=mesh,
        in_specs=(P(("groups", "blk"), "sub", None), P(("groups", "blk"), "sub", None), P("groups")),
        out_specs=P(("groups", "blk"), "sub", None),
        check_vma=False,
    )
```
